128 devices in a mesh: row: 8 (over y, x_lo), col: 16 (over z, x_hi, core).
Axes of the slice: x: 4 (x_hi: 2, x_lo: 2; x = x_hi * 2 + x_lo), y: 4, z: 4, core: 2. Of those that a mesh axis runs over, the one named last changes fastest.
Arguments:
- gains: float32 [512, 8, 256], P(('row', 'col')), may hold values from -6 to 6
- coherency: bfloat16 [512, 512, 8, 1, 256], P('row', 'col'), may hold values from -6 to 6
- cotangent: bfloat16 [512, 512, 8, 1, 8], P('row', 'col'), may hold values from -0.099609375 to 0.099609375
- flags: int32 [512, 512, 1], P('row', 'col'), may hold values 0 or 1
- station_slot: int32 [512], replicated, may hold values from 0 to 511, as said below
Outputs:
- gain_grad: float32 [512, 8, 256], P(('row', 'col'))
The draws below stay inside these ranges and needn't reach their ends.
Inputs may be any that keep to these rules, and one draw needn't show every extreme that they name: `station_slot`: each station appears in exactly one slot; in every aligned block of 4 consecutive slots the stations lie with 4 different holders, station s being held by the device of index s // 4 in the order of row+col.
All inputs are finite; a program needn't handle non-finite values. No bound on the sum of `flags` on one device may be relied on, other than what follows from the above.
Results may differ from the reference program's by a relative error of at most 0.0003.
Values sent between devices are 32-bit elements; how exact they have to be, the bound alone decides.
No kernel may reach another device: no remote copies, remote signals or barrier semaphores. Data moves between devices by JAX's collectives and lax.ppermute only.
A program may use at most 128 MiB of HBM per device.

```python
import jax
import jax.numpy as jnp
from jax import lax

S = 512
GROUPS = 128
SD = 4
DIR = 32
CH = 8
TI = 1


def draw_station_slot(key, part):
    keys = jax.random.split(jax.random.fold_in(key, 17), 3)
    order = jax.random.permutation(keys[0], GROUPS).astype(jnp.int32)
    within = jax.random.randint(keys[1], (GROUPS,), 0, SD).astype(jnp.int32)
    offset = jax.random.randint(keys[2], (GROUPS,), 0, SD).astype(jnp.int32)
    stride = GROUPS // SD
    blocks = jnp.arange(GROUPS, dtype=jnp.int32)[:, None]
    places = jnp.arange(SD, dtype=jnp.int32)[None, :]
    holder = (order[blocks] + places * stride) % GROUPS
    number = (places + within[holder]) % SD
    station = holder * SD + number
    position = (places + offset[blocks]) % SD
    block_ids = jnp.broadcast_to(blocks, (GROUPS, SD))
    filled = jnp.zeros((GROUPS, SD), jnp.int32).at[block_ids, position].set(station)
    return filled.reshape(GROUPS * SD).astype(jnp.int32)


def plant(array, key, low, largest):
    shape = array.shape
    spot = [jax.random.randint(jax.random.fold_in(key, axis), (), 0, shape[axis]) for axis in range(len(shape))]
    array = array.at[tuple(spot)].set(low)
    longest = shape.index(max(shape))
    spot[longest] = (spot[longest] + 1) % shape[longest]
    return array.at[tuple(spot)].set(largest)


def level_of(stream_key, extent, cuts, low, top_value):
    def one(axis_at, blocks):
        heights = jax.random.uniform(jax.random.fold_in(jax.random.fold_in(stream_key, 6), axis_at), (blocks,), jnp.float32, low / len(cuts), top_value / len(cuts))
        return jnp.repeat(jnp.exp(heights), extent[axis_at] // blocks).reshape((-1,) + (1,) * (len(extent) - axis_at - 1))

    gain = one(*cuts[0])
    for cut in cuts[1:]:
        gain = gain * one(*cut)
    return gain


def centred(rng, shape, spread, most, shards=(), held_as=jnp.bfloat16):
    entries = jax.random.normal(rng, shape, jnp.float32) * spread
    if len(shards) > 0:
        entries = level_of(rng, shape, shards, -0.22, 0.18) * entries
    return jnp.clip(entries, min=-most, max=most).astype(held_as)


def setup_inputs(seed: int = 0) -> dict:
    seeds = jax.random.split(jax.random.key(seed), 6)
    return {
        "gains": centred(seeds[0], (S, CH, 8 * DIR), 1.0, 6.0, ((0, 128),), jnp.float32),
        "coherency": centred(seeds[1], (S, S, CH, TI, 8 * DIR), 1.0, 6.0, ((0, 8), (1, 16))),
        "cotangent": centred(seeds[2], (S, S, CH, TI, 8), 0.016, 0.099609375, ((0, 8), (1, 16))),
        "flags": plant((jax.random.randint(seeds[3], (S, S, TI), 0, 4) < 3).astype(jnp.int32), jax.random.fold_in(seeds[3], 1), 0, 1),
        "station_slot": draw_station_slot(jax.random.fold_in(seeds[5], 71), 0),
    }


def complex_product(first, second):
    return (first[0] * second[0] - first[1] * second[1], first[0] * second[1] + first[1] * second[0])


def complex_sum(first, second):
    return (first[0] + second[0], first[1] + second[1])


def conjugate(element):
    return (element[0], -element[1])


def jones_product(first, second):
    return [complex_sum(complex_product(first[2 * row_index], second[column]), complex_product(first[2 * row_index + 1], second[2 + column])) for row_index in (0, 1) for column in (0, 1)]


def hermitian(matrix):
    return [conjugate(matrix[0]), conjugate(matrix[2]), conjugate(matrix[1]), conjugate(matrix[3])]


def as_complex(parts):
    return [(parts[0], parts[1]), (parts[2], parts[3]), (parts[4], parts[5]), (parts[6], parts[7])]


def as_parts(matrix):
    return [number for element in matrix for number in element]


def block_gradients(coherency, cotangent, flags, row_gains, col_gains):
    shape = coherency.shape
    directions = shape[4] // 8
    coherence = coherency.reshape(shape[:4] + (8, directions))
    weight = flags.astype(jnp.float32)[:, :, None, :, None]
    residual = as_complex([cotangent[..., component].astype(jnp.float32)[..., None] * weight for component in range(8)])
    model_parts = as_complex([coherence[..., component, :].astype(jnp.float32) for component in range(8)])
    row_split = row_gains.reshape(row_gains.shape[0], row_gains.shape[1], 8, directions)
    col_split = col_gains.reshape(col_gains.shape[0], col_gains.shape[1], 8, directions)
    row_jones = as_complex([row_split[:, None, :, None, component, :] for component in range(8)])
    col_jones = as_complex([col_split[None, :, :, None, component, :] for component in range(8)])
    outgoing = jones_product(jones_product(residual, col_jones), hermitian(model_parts))
    row_side = jnp.stack([jnp.sum(part, axis=(1, 3)) for part in as_parts(outgoing)], axis=2)
    incoming = jones_product(jones_product(hermitian(residual), row_jones), model_parts)
    col_side = jnp.stack([jnp.sum(part, axis=(0, 3)) for part in as_parts(incoming)], axis=2)
    return row_side.reshape(row_gains.shape), col_side.reshape(col_gains.shape)


def reference(gains, coherency, cotangent, flags, station_slot):
    slot_gains = jnp.take(gains, station_slot, axis=0)
    block_rows = 16
    stations = gains.shape[0]

    def accumulate(totals, block_index):
        start = (block_index * block_rows).astype(jnp.int32)
        coher_rows = lax.dynamic_slice_in_dim(coherency, start, block_rows, 0)
        cotan_rows = lax.dynamic_slice_in_dim(cotangent, start, block_rows, 0)
        flag_rows = lax.dynamic_slice_in_dim(flags, start, block_rows, 0)
        gain_rows = lax.dynamic_slice_in_dim(slot_gains, start, block_rows, 0)
        row_side, col_side = block_gradients(coher_rows, cotan_rows, flag_rows, gain_rows, slot_gains)
        return totals + col_side, row_side

    indices = jnp.arange(stations // block_rows, dtype=jnp.int32)
    col_total, row_blocks = lax.scan(accumulate, jnp.zeros(gains.shape, gains.dtype), indices)
    slot_grad = row_blocks.reshape(gains.shape) + col_total
    return jnp.zeros(gains.shape, gains.dtype).at[station_slot].set(slot_grad)
```

```python
import functools

import jax
import jax.numpy as jnp
from jax import lax
from jax.experimental import pallas as pl
from jax.experimental.pallas import tpu as pltpu
from jax.sharding import PartitionSpec as P

LANES = 128
PER_STEP = 4


def exchanged(x, axis):
    return lax.all_to_all(x, axis, split_axis=0, concat_axis=0, tiled=True)


def swapped(x, group, even):
    return jnp.where(even, pltpu.roll(x, LANES - group, 1), pltpu.roll(x, group, 1))


def summed_groups(x, group):
    half = x + pltpu.roll(x, 2 * group, 1)
    return half + pltpu.roll(half, group, 1)


def replicas(x, group, place):
    kept = jnp.where(place, x, 0.0)
    return summed_groups(kept, group)


def gradients_kernel(
    row_gains, col_gains, residual, coherency, row_side, col_side, col_parts, col_sums, *, group
):
    step = pl.program_id(0)
    per_step, col_count, channels, _ = coherency.shape
    lane = lax.broadcasted_iota(jnp.int32, (channels, LANES), 1)
    index = lane // group
    even = index % 2 == 0
    sign = jnp.where(even, -1.0, 1.0).astype(jnp.float32)

    @pl.when(step == 0)
    def _():
        col_sums[...] = jnp.zeros(col_sums.shape, col_sums.dtype)

        def prepare(k, carry):
            for b in (0, 1):
                own = col_gains[k, :, b * LANES : (b + 1) * LANES]
                col_parts[k, b] = own
                col_parts[k, 2 + b] = sign * swapped(own, group, even)
            return carry

        lax.fori_loop(0, col_count, prepare, 0)

    def one_row(i, carry):
        gains = [row_gains[i, :, b * LANES : (b + 1) * LANES] for b in (0, 1)]
        real = [[replicas(gains[b], group, index == 2 * s) for s in (0, 1)] for b in (0, 1)]
        imag = [[sign * replicas(gains[b], group, index == 2 * s + 1) for s in (0, 1)] for b in (0, 1)]
        weights = residual[i].astype(jnp.float32)
        zero = jnp.zeros((channels, LANES), jnp.float32)
        re_sum = [[zero, zero], [zero, zero]]
        im_sum = [[zero, zero], [zero, zero]]
        for k in range(col_count):
            model = coherency[i, k].astype(jnp.float32)
            m = [model[:, :LANES], model[:, LANES:]]
            sm = [swapped(m[0], group, even), swapped(m[1], group, even)]
            at = k * 8
            g = [
                jnp.broadcast_to(weights[:, at + n : at + n + 1], (channels, LANES))
                for n in range(8)
            ]
            for a in (0, 1):
                product = (
                    g[4 * a] * col_parts[k, 0]
                    + g[4 * a + 1] * col_parts[k, 2]
                    + g[4 * a + 2] * col_parts[k, 1]
                    + g[4 * a + 3] * col_parts[k, 3]
                )
                for c in (0, 1):
                    re_sum[a][c] = re_sum[a][c] + product * m[c]
                    im_sum[a][c] = im_sum[a][c] + product * sm[c]
            t = [
                real[b][0] * m[0] + imag[b][0] * sm[0] + real[b][1] * m[1] + imag[b][1] * sm[1]
                for b in (0, 1)
            ]
            for a in (0, 1):
                col_sums[k, a] += g[2 * a] * t[0] + g[4 + 2 * a] * t[1]
                col_sums[k, 2 + a] += g[2 * a + 1] * t[0] + g[4 + 2 * a + 1] * t[1]
        for a in (0, 1):
            parts = []
            for c in (0, 1):
                parts.append(summed_groups(re_sum[a][c], group))
                parts.append(summed_groups(sign * im_sum[a][c], group))
            joined = parts[3]
            for n in (0, 1, 2):
                joined = jnp.where(index == n, parts[n], joined)
            row_side[i, :, a * LANES : (a + 1) * LANES] = joined
        return carry

    lax.fori_loop(0, per_step, one_row, 0)

    @pl.when(step == pl.num_programs(0) - 1)
    def _():
        def finish(k, carry):
            for a in (0, 1):
                turned = sign * swapped(col_sums[k, 2 + a], group, even)
                col_side[k, :, a * LANES : (a + 1) * LANES] = col_sums[k, a] - turned
            return carry

        lax.fori_loop(0, col_count, finish, 0)


def block_gradients(coherency, residual, row_gains, col_gains, interpret=False):
    rows, cols, channels, width = coherency.shape
    return pl.pallas_call(
        functools.partial(gradients_kernel, group=width // 8),
        grid=(rows // PER_STEP,),
        in_specs=[
            pl.BlockSpec((PER_STEP, channels, width), lambda s: (s, 0, 0)),
            pl.BlockSpec((cols, channels, width), lambda s: (0, 0, 0)),
            pl.BlockSpec((PER_STEP, channels, cols * 8), lambda s: (s, 0, 0)),
            pl.BlockSpec((PER_STEP, cols, channels, width), lambda s: (s, 0, 0, 0)),
        ],
        out_specs=[
            pl.BlockSpec((PER_STEP, channels, width), lambda s: (s, 0, 0)),
            pl.BlockSpec((cols, channels, width), lambda s: (0, 0, 0)),
        ],
        out_shape=[
            jax.ShapeDtypeStruct((rows, channels, width), jnp.float32),
            jax.ShapeDtypeStruct((cols, channels, width), jnp.float32),
        ],
        scratch_shapes=[
            pltpu.VMEM((cols, 4, channels, LANES), jnp.float32),
            pltpu.VMEM((cols, 4, channels, LANES), jnp.float32),
        ],
        compiler_params=pltpu.CompilerParams(dimension_semantics=("arbitrary",)),
        interpret=interpret,
        name="gradients",
    )(row_gains, col_gains, residual, coherency)


def weighted(cotangent, flags):
    rows, cols, channels = cotangent.shape[:3]
    kept = cotangent[:, :, :, 0, :] * flags.astype(cotangent.dtype)[:, :, :, None]
    return jnp.transpose(kept, (0, 2, 1, 3)).reshape(rows, channels, cols * 8)


def one_hot_product(table, values, dims):
    return lax.dot_general(
        table,
        values,
        (dims, ((), ())),
        precision=lax.Precision.HIGHEST,
        preferred_element_type=jnp.float32,
    )


def shards(gains, coherency, cotangent, flags, station_slot):
    stations = station_slot.shape[0]
    share, channels, width = gains.shape
    row_total = lax.axis_size("row")
    col_total = lax.axis_size("col")
    groups = row_total * col_total
    rows, cols = coherency.shape[:2]
    col_start = lax.axis_index("col") * cols

    by_channel = jnp.transpose(gains, (1, 0, 2))
    outward = jnp.broadcast_to(
        by_channel[:, None], (row_total, col_total, share, width)
    ).reshape(groups, share, width)
    channel_gains = exchanged(outward, ("row", "col")).reshape(stations, width)

    identity = jnp.arange(stations, dtype=jnp.int32)[None, :]
    table = (station_slot[:, None] == identity).astype(jnp.float32)
    slot_gains = one_hot_product(table, channel_gains, ((1,), (0,)))
    of_rows = slot_gains.reshape(row_total, rows, width)
    of_col = lax.dynamic_slice_in_dim(slot_gains, col_start, cols)
    of_cols = jnp.broadcast_to(of_col[None], (row_total, cols, width))
    needed = exchanged(jnp.concatenate([of_rows, of_cols], axis=1), "row")
    by_slot = jnp.transpose(needed, (1, 0, 2))

    row_side, col_side = block_gradients(
        coherency[:, :, :, 0, :], weighted(cotangent, flags), by_slot[:rows], by_slot[rows:]
    )

    both = jnp.transpose(jnp.concatenate([row_side, col_side], axis=0), (1, 0, 2))
    arrived = exchanged(both, "row")
    of_slots = arrived[:, :rows].reshape(stations, width)
    col_sum = jnp.sum(arrived[:, rows:], axis=0)
    mine = lax.dynamic_slice_in_dim(of_slots, col_start, cols)
    of_slots = lax.dynamic_update_slice_in_dim(of_slots, mine + col_sum, col_start, 0)
    of_stations = one_hot_product(table, of_slots, ((0,), (0,)))
    homeward = exchanged(of_stations.reshape(groups, share, width), ("row", "col"))
    total = jnp.sum(homeward.reshape(row_total, col_total, share, width), axis=1)
    return jnp.transpose(total, (1, 0, 2))


def solution(mesh):
    placed = (
        P(("row", "col"), None, None),
        P("row", "col", None, None, None),
        P("row", "col", None, None, None),
        P("row", "col", None),
        P(),
    )
    return jax.shard_map(
        shards, mesh=mesh, in_specs=placed, out_specs=P(("row", "col"), None, None), check_vma=False
    )
```

```python
import functools

import jax
import jax.numpy as jnp
from jax import lax
from jax.experimental import pallas as pl
from jax.experimental.pallas import tpu as pltpu
from jax.sharding import PartitionSpec as P

LANES = 128
PER_STEP = 4
UNROLL = 16


def exchanged(x, axis):
    return lax.all_to_all(x, axis, split_axis=0, concat_axis=0, tiled=True)


def swapped(x, group, even):
    return jnp.where(even, pltpu.roll(x, LANES - group, 1), pltpu.roll(x, group, 1))


def summed_groups(x, group):
    half = x + pltpu.roll(x, 2 * group, 1)
    return half + pltpu.roll(half, group, 1)


def replicas(x, group, place):
    kept = jnp.where(place, x, 0.0)
    return summed_groups(kept, group)


def gradients_kernel(
    row_gains,
    col_gains,
    residual,
    coherency,
    spread,
    swap,
    row_side,
    col_side,
    col_parts,
    col_sums,
    *,
    group,
):
    step = pl.program_id(0)
    per_step, col_count, channels, _ = coherency.shape
    lane = lax.broadcasted_iota(jnp.int32, (channels, LANES), 1)
    index = lane // group
    even = index % 2 == 0
    sign = jnp.where(even, -1.0, 1.0).astype(jnp.float32)

    @pl.when(step == 0)
    def _():
        col_sums[...] = jnp.zeros(col_sums.shape, col_sums.dtype)

        def prepare(k, carry):
            for b in (0, 1):
                own = col_gains[k, :, b * LANES : (b + 1) * LANES]
                col_parts[k, b] = own
                col_parts[k, 2 + b] = sign * swapped(own, group, even)
            return carry

        lax.fori_loop(0, col_count, prepare, 0)

    def one_row(i, carry):
        gains = [row_gains[i, :, b * LANES : (b + 1) * LANES] for b in (0, 1)]
        real = [[replicas(gains[b], group, index == 2 * s) for s in (0, 1)] for b in (0, 1)]
        imag = [[sign * replicas(gains[b], group, index == 2 * s + 1) for s in (0, 1)] for b in (0, 1)]
        zero = jnp.zeros((channels, LANES), jnp.float32)

        def some_cols(block, sums):
            sums = list(sums)
            weights = jnp.dot(
                residual[i, block], spread[...], preferred_element_type=jnp.float32
            )
            models = coherency[i, pl.ds(block * UNROLL, UNROLL)].reshape(
                UNROLL * channels, 2 * LANES
            )
            turned = jnp.dot(models, swap[...], preferred_element_type=jnp.float32)
            for j in range(UNROLL):
                k = block * UNROLL + j
                at = slice(j * channels, (j + 1) * channels)
                model = models[at].astype(jnp.float32)
                m = [model[:, :LANES], model[:, LANES:]]
                sm = [turned[at, :LANES], turned[at, LANES:]]
                g = [weights[at, n * LANES : (n + 1) * LANES] for n in range(8)]
                for a in (0, 1):
                    product = (
                        g[4 * a] * col_parts[k, 0]
                        + g[4 * a + 1] * col_parts[k, 2]
                        + g[4 * a + 2] * col_parts[k, 1]
                        + g[4 * a + 3] * col_parts[k, 3]
                    )
                    for c in (0, 1):
                        to = 4 * a + 2 * c
                        sums[to] = sums[to] + product * m[c]
                        sums[to + 1] = sums[to + 1] + product * sm[c]
                t = [
                    real[b][0] * m[0] + imag[b][0] * sm[0] + real[b][1] * m[1] + imag[b][1] * sm[1]
                    for b in (0, 1)
                ]
                for a in (0, 1):
                    col_sums[k, a] += g[2 * a] * t[0] + g[4 + 2 * a] * t[1]
                    col_sums[k, 2 + a] += g[2 * a + 1] * t[0] + g[4 + 2 * a + 1] * t[1]
            return tuple(sums)

        sums = lax.fori_loop(0, col_count // UNROLL, some_cols, (zero,) * 8)
        for a in (0, 1):
            parts = []
            for c in (0, 1):
                parts.append(summed_groups(sums[4 * a + 2 * c], group))
                parts.append(summed_groups(sign * sums[4 * a + 2 * c + 1], group))
            joined = parts[3]
            for n in (0, 1, 2):
                joined = jnp.where(index == n, parts[n], joined)
            row_side[i, :, a * LANES : (a + 1) * LANES] = joined
        return carry

    lax.fori_loop(0, per_step, one_row, 0)

    @pl.when(step == pl.num_programs(0) - 1)
    def _():
        def finish(k, carry):
            for a in (0, 1):
                turned = sign * swapped(col_sums[k, 2 + a], group, even)
                col_side[k, :, a * LANES : (a + 1) * LANES] = col_sums[k, a] - turned
            return carry

        lax.fori_loop(0, col_count, finish, 0)


def block_gradients(coherency, residual, row_gains, col_gains, interpret=False):
    rows, cols, channels, width = coherency.shape
    group = width // 8
    lane = jnp.arange(8 * LANES, dtype=jnp.int32)
    spread = (lane[None, :8] == (lane[:, None] // LANES)).T.astype(jnp.bfloat16)
    part = lane[:width]
    partner = part + jnp.where(part // group % 2 == 0, group, -group)
    swap = (part[:, None] == partner[None, :]).astype(jnp.bfloat16)
    return pl.pallas_call(
        functools.partial(gradients_kernel, group=width // 8),
        grid=(rows // PER_STEP,),
        in_specs=[
            pl.BlockSpec((PER_STEP, channels, width), lambda s: (s, 0, 0)),
            pl.BlockSpec((cols, channels, width), lambda s: (0, 0, 0)),
            pl.BlockSpec((PER_STEP, cols // UNROLL, UNROLL * channels, 8), lambda s: (s, 0, 0, 0)),
            pl.BlockSpec((PER_STEP, cols, channels, width), lambda s: (s, 0, 0, 0)),
            pl.BlockSpec((8, 8 * LANES), lambda s: (0, 0)),
            pl.BlockSpec((width, width), lambda s: (0, 0)),
        ],
        out_specs=[
            pl.BlockSpec((PER_STEP, channels, width), lambda s: (s, 0, 0)),
            pl.BlockSpec((cols, channels, width), lambda s: (0, 0, 0)),
        ],
        out_shape=[
            jax.ShapeDtypeStruct((rows, channels, width), jnp.float32),
            jax.ShapeDtypeStruct((cols, channels, width), jnp.float32),
        ],
        scratch_shapes=[
            pltpu.VMEM((cols, 4, channels, LANES), jnp.float32),
            pltpu.VMEM((cols, 4, channels, LANES), jnp.float32),
        ],
        compiler_params=pltpu.CompilerParams(dimension_semantics=("arbitrary",)),
        interpret=interpret,
        name="gradients",
    )(row_gains, col_gains, residual, coherency, spread, swap)


def weighted(cotangent, flags):
    rows, cols, channels = cotangent.shape[:3]
    kept = cotangent[:, :, :, 0, :] * flags.astype(cotangent.dtype)[:, :, :, None]
    return kept.reshape(rows, cols // UNROLL, UNROLL * channels, 8)


def one_hot_product(table, values, dims):
    return lax.dot_general(
        table,
        values,
        (dims, ((), ())),
        precision=lax.Precision.HIGHEST,
        preferred_element_type=jnp.float32,
    )


def shards(gains, coherency, cotangent, flags, station_slot):
    stations = station_slot.shape[0]
    share, channels, width = gains.shape
    row_total = lax.axis_size("row")
    col_total = lax.axis_size("col")
    groups = row_total * col_total
    rows, cols = coherency.shape[:2]
    col_start = lax.axis_index("col") * cols

    by_channel = jnp.transpose(gains, (1, 0, 2))
    outward = jnp.broadcast_to(
        by_channel[:, None], (row_total, col_total, share, width)
    ).reshape(groups, share, width)
    channel_gains = exchanged(outward, ("row", "col")).reshape(stations, width)

    identity = jnp.arange(stations, dtype=jnp.int32)[None, :]
    table = (station_slot[:, None] == identity).astype(jnp.float32)
    slot_gains = one_hot_product(table, channel_gains, ((1,), (0,)))
    of_rows = slot_gains.reshape(row_total, rows, width)
    of_col = lax.dynamic_slice_in_dim(slot_gains, col_start, cols)
    of_cols = jnp.broadcast_to(of_col[None], (row_total, cols, width))
    needed = exchanged(jnp.concatenate([of_rows, of_cols], axis=1), "row")
    by_slot = jnp.transpose(needed, (1, 0, 2))

    row_side, col_side = block_gradients(
        coherency[:, :, :, 0, :], weighted(cotangent, flags), by_slot[:rows], by_slot[rows:]
    )

    both = jnp.transpose(jnp.concatenate([row_side, col_side], axis=0), (1, 0, 2))
    arrived = exchanged(both, "row")
    of_slots = arrived[:, :rows].reshape(stations, width)
    col_sum = jnp.sum(arrived[:, rows:], axis=0)
    mine = lax.dynamic_slice_in_dim(of_slots, col_start, cols)
    of_slots = lax.dynamic_update_slice_in_dim(of_slots, mine + col_sum, col_start, 0)
    of_stations = one_hot_product(table, of_slots, ((0,), (0,)))
    homeward = exchanged(of_stations.reshape(groups, share, width), ("row", "col"))
    total = jnp.sum(homeward.reshape(row_total, col_total, share, width), axis=1)
    return jnp.transpose(total, (1, 0, 2))


def solution(mesh):
    placed = (
        P(("row", "col"), None, None),
        P("row", "col", None, None, None),
        P("row", "col", None, None, None),
        P("row", "col", None),
        P(),
    )
    return jax.shard_map(
        shards, mesh=mesh, in_specs=placed, out_specs=P(("row", "col"), None, None), check_vma=False
    )
```

```python
import functools

import jax
import jax.numpy as jnp
from jax import lax
from jax.experimental import pallas as pl
from jax.experimental.pallas import tpu as pltpu
from jax.sharding import PartitionSpec as P

LANES = 128
PER_STEP = 8
BATCH = 8


def exchanged(x, axis):
    return lax.all_to_all(x, axis, split_axis=0, concat_axis=0, tiled=True)


def swapped(x, group, even):
    return jnp.where(even, pltpu.roll(x, LANES - group, 1), pltpu.roll(x, group, 1))


def summed_groups(x, group):
    half = x + pltpu.roll(x, 2 * group, 1)
    return half + pltpu.roll(half, group, 1)


def replicas(x, group, place):
    kept = jnp.where(place, x, 0.0)
    return summed_groups(kept, group)


def swap_kernel(coherency, swap, turned):
    rows = coherency.shape[0] * coherency.shape[1] * coherency.shape[2]
    flat = coherency[...].reshape(rows, coherency.shape[3])
    product = jnp.dot(flat, swap[...], preferred_element_type=jnp.float32)
    turned[...] = product.astype(turned.dtype).reshape(turned.shape)


def swapped_pairs(coherency, interpret=False):
    rows, cols, channels, width = coherency.shape
    group = width // 8
    part = jnp.arange(width, dtype=jnp.int32)
    partner = part + jnp.where(part // group % 2 == 0, group, -group)
    swap = (part[:, None] == partner[None, :]).astype(coherency.dtype)
    block = pl.BlockSpec((PER_STEP, cols, channels, width), lambda s: (s, 0, 0, 0))
    return pl.pallas_call(
        swap_kernel,
        grid=(rows // PER_STEP,),
        in_specs=[block, pl.BlockSpec((width, width), lambda s: (0, 0))],
        out_specs=block,
        out_shape=jax.ShapeDtypeStruct(coherency.shape, coherency.dtype),
        compiler_params=pltpu.CompilerParams(dimension_semantics=("arbitrary",)),
        cost_estimate=pl.CostEstimate(
            flops=2 * width * coherency.size, bytes_accessed=4 * coherency.size, transcendentals=0
        ),
        interpret=interpret,
        name="swap",
    )(coherency, swap)


def gradients_kernel(
    row_gains,
    col_gains,
    residual,
    coherency,
    turned,
    spread,
    row_side,
    col_side,
    row_parts,
    row_sums,
    col_parts,
    col_sums,
    weights_even,
    weights_odd,
    *,
    group,
):
    step = pl.program_id(0)
    per_step, col_count, channels, _ = coherency.shape
    row_count = row_gains.shape[0]
    lane = lax.broadcasted_iota(jnp.int32, (channels, LANES), 1)
    index = lane // group
    even = index % 2 == 0
    sign = jnp.where(even, -1.0, 1.0).astype(jnp.float32)

    @pl.when(step == 0)
    def _():
        col_sums[...] = jnp.zeros(col_sums.shape, col_sums.dtype)

        def prepare_cols(block, carry):
            for j in range(BATCH):
                k = block * BATCH + j
                for b in (0, 1):
                    own = col_gains[k, :, b * LANES : (b + 1) * LANES]
                    col_parts[k, b] = own
                    col_parts[k, 2 + b] = sign * swapped(own, group, even)
            return carry

        lax.fori_loop(0, col_count // BATCH, prepare_cols, 0)

        def prepare_rows(block, carry):
            for j in range(BATCH):
                i = block * BATCH + j
                for b in (0, 1):
                    own = row_gains[i, :, b * LANES : (b + 1) * LANES]
                    for n in range(4):
                        copies = replicas(own, group, index == n)
                        row_parts[i, 4 * b + n] = copies if n % 2 == 0 else sign * copies
            return carry

        lax.fori_loop(0, row_count // BATCH, prepare_rows, 0)

    def spread_out(i, weights):
        weights[...] = lax.dot_general(
            residual[i], spread[...], (((0,), (0,)), ((), ())), preferred_element_type=jnp.float32
        )

    def one_row(i, weights):
        row = step * per_step + i
        zero = jnp.zeros((channels, LANES), jnp.float32)
        sums = [zero] * 8
        for k in range(col_count):
            at = slice(k * channels, (k + 1) * channels)
            model = coherency[i, k].astype(jnp.float32)
            other = turned[i, k].astype(jnp.float32)
            m = [model[:, :LANES], model[:, LANES:]]
            sm = [other[:, :LANES], other[:, LANES:]]
            g = [weights[at, n * LANES : (n + 1) * LANES] for n in range(8)]
            for a in (0, 1):
                product = (
                    g[4 * a] * col_parts[k, 0]
                    + g[4 * a + 1] * col_parts[k, 2]
                    + g[4 * a + 2] * col_parts[k, 1]
                    + g[4 * a + 3] * col_parts[k, 3]
                )
                for c in (0, 1):
                    to = 4 * a + 2 * c
                    sums[to] = sums[to] + product * m[c]
                    sums[to + 1] = sums[to + 1] + product * sm[c]
            t = [
                row_parts[row, 4 * b] * m[0]
                + row_parts[row, 4 * b + 1] * sm[0]
                + row_parts[row, 4 * b + 2] * m[1]
                + row_parts[row, 4 * b + 3] * sm[1]
                for b in (0, 1)
            ]
            for a in (0, 1):
                col_sums[k, a] += g[2 * a] * t[0] + g[4 + 2 * a] * t[1]
                col_sums[k, 2 + a] += g[2 * a + 1] * t[0] + g[4 + 2 * a + 1] * t[1]
        for n in range(8):
            row_sums[row, n] = sums[n]

    spread_out(0, weights_even)

    def two_rows(half, carry):
        i = 2 * half
        spread_out(i + 1, weights_odd)
        one_row(i, weights_even)
        spread_out(jnp.minimum(i + 2, per_step - 1), weights_even)
        one_row(i + 1, weights_odd)
        return carry

    lax.fori_loop(0, per_step // 2, two_rows, 0)

    @pl.when(step == pl.num_programs(0) - 1)
    def _():
        def finish_rows(block, carry):
            for j in range(BATCH):
                i = block * BATCH + j
                for a in (0, 1):
                    joined = None
                    for n in range(4):
                        own = row_sums[i, 4 * a + n]
                        part = summed_groups(own if n % 2 == 0 else sign * own, group)
                        joined = part if n == 0 else jnp.where(index == n, part, joined)
                    row_side[i, :, a * LANES : (a + 1) * LANES] = joined
            return carry

        lax.fori_loop(0, row_count // BATCH, finish_rows, 0)

        def finish_cols(block, carry):
            for j in range(BATCH):
                k = block * BATCH + j
                for a in (0, 1):
                    back = sign * swapped(col_sums[k, 2 + a], group, even)
                    col_side[k, :, a * LANES : (a + 1) * LANES] = col_sums[k, a] - back
            return carry

        lax.fori_loop(0, col_count // BATCH, finish_cols, 0)


def block_gradients(coherency, turned, residual, row_gains, col_gains, interpret=False):
    rows, cols, channels, width = coherency.shape
    lane = jnp.arange(8 * LANES, dtype=jnp.int32)
    spread = (lane[None, :8] == (lane[:, None] // LANES)).T.astype(jnp.bfloat16)
    block = pl.BlockSpec((PER_STEP, cols, channels, width), lambda s: (s, 0, 0, 0))
    every_row = pl.BlockSpec((rows, channels, width), lambda s: (0, 0, 0))
    every_col = pl.BlockSpec((cols, channels, width), lambda s: (0, 0, 0))
    return pl.pallas_call(
        functools.partial(gradients_kernel, group=width // 8),
        grid=(rows // PER_STEP,),
        in_specs=[
            every_row,
            every_col,
            pl.BlockSpec((PER_STEP, 8, cols * channels), lambda s: (s, 0, 0)),
            block,
            block,
            pl.BlockSpec((8, 8 * LANES), lambda s: (0, 0)),
        ],
        out_specs=[every_row, every_col],
        out_shape=[
            jax.ShapeDtypeStruct((rows, channels, width), jnp.float32),
            jax.ShapeDtypeStruct((cols, channels, width), jnp.float32),
        ],
        scratch_shapes=[
            pltpu.VMEM((rows, 8, channels, LANES), jnp.float32),
            pltpu.VMEM((rows, 8, channels, LANES), jnp.float32),
            pltpu.VMEM((cols, 4, channels, LANES), jnp.float32),
            pltpu.VMEM((cols, 4, channels, LANES), jnp.float32),
            pltpu.VMEM((cols * channels, 8 * LANES), jnp.float32),
            pltpu.VMEM((cols * channels, 8 * LANES), jnp.float32),
        ],
        compiler_params=pltpu.CompilerParams(dimension_semantics=("arbitrary",)),
        interpret=interpret,
        name="gradients",
    )(row_gains, col_gains, residual, coherency, turned, spread)


def weighted(cotangent, flags):
    rows, cols, channels = cotangent.shape[:3]
    kept = cotangent[:, :, :, 0, :] * flags.astype(cotangent.dtype)[:, :, :, None]
    return jnp.transpose(kept, (0, 3, 1, 2)).reshape(rows, 8, cols * channels)


def one_hot_product(table, values, dims):
    return lax.dot_general(
        table,
        values,
        (dims, ((), ())),
        precision=lax.Precision.HIGHEST,
        preferred_element_type=jnp.float32,
    )


def shards(gains, coherency, cotangent, flags, station_slot):
    stations = station_slot.shape[0]
    share, channels, width = gains.shape
    row_total = lax.axis_size("row")
    col_total = lax.axis_size("col")
    groups = row_total * col_total
    rows, cols = coherency.shape[:2]
    col_start = lax.axis_index("col") * cols

    by_channel = jnp.transpose(gains, (1, 0, 2))
    outward = jnp.broadcast_to(
        by_channel[:, None], (row_total, col_total, share, width)
    ).reshape(groups, share, width)
    channel_gains = exchanged(outward, ("row", "col"))
    models = coherency[:, :, :, 0, :]
    channel_gains, turned = lax.optimization_barrier((channel_gains, swapped_pairs(models)))
    channel_gains = channel_gains.reshape(stations, width)

    identity = jnp.arange(stations, dtype=jnp.int32)[None, :]
    table = (station_slot[:, None] == identity).astype(jnp.float32)
    slot_gains = one_hot_product(table, channel_gains, ((1,), (0,)))
    of_rows = slot_gains.reshape(row_total, rows, width)
    of_col = lax.dynamic_slice_in_dim(slot_gains, col_start, cols)
    of_cols = jnp.broadcast_to(of_col[None], (row_total, cols, width))
    needed = exchanged(jnp.concatenate([of_rows, of_cols], axis=1), "row")
    by_slot = jnp.transpose(needed, (1, 0, 2))

    row_side, col_side = block_gradients(
        models,
        turned,
        weighted(cotangent, flags),
        by_slot[:rows],
        by_slot[rows:],
    )

    both = jnp.transpose(jnp.concatenate([row_side, col_side], axis=0), (1, 0, 2))
    arrived = exchanged(both, "row")
    of_slots = arrived[:, :rows].reshape(stations, width)
    col_sum = jnp.sum(arrived[:, rows:], axis=0)
    mine = lax.dynamic_slice_in_dim(of_slots, col_start, cols)
    of_slots = lax.dynamic_update_slice_in_dim(of_slots, mine + col_sum, col_start, 0)
    of_stations = one_hot_product(table, of_slots, ((0,), (0,)))
    homeward = exchanged(of_stations.reshape(groups, share, width), ("row", "col"))
    total = jnp.sum(homeward.reshape(row_total, col_total, share, width), axis=1)
    return jnp.transpose(total, (1, 0, 2))


def solution(mesh):
    placed = (
        P(("row", "col"), None, None),
        P("row", "col", None, None, None),
        P("row", "col", None, None, None),
        P("row", "col", None),
        P(),
    )
    return jax.shard_map(
        shards, mesh=mesh, in_specs=placed, out_specs=P(("row", "col"), None, None), check_vma=False
    )
```

```python
import functools

import jax
import jax.numpy as jnp
from jax import lax
from jax.experimental import pallas as pl
from jax.experimental.pallas import tpu as pltpu
from jax.sharding import PartitionSpec as P

LANES = 128
PER_STEP = 8
SWAP_STEP = 16
BATCH = 8


def exchanged(x, axis):
    return lax.all_to_all(x, axis, split_axis=0, concat_axis=0, tiled=True)


def swapped(x, group, even):
    return jnp.where(even, pltpu.roll(x, LANES - group, 1), pltpu.roll(x, group, 1))


def summed_groups(x, group):
    half = x + pltpu.roll(x, 2 * group, 1)
    return half + pltpu.roll(half, group, 1)


def replicas(x, group, place):
    kept = jnp.where(place, x, 0.0)
    return summed_groups(kept, group)


def swap_kernel(coherency, swap, turned):
    rows = coherency.shape[0] * coherency.shape[1] * coherency.shape[2]
    flat = coherency[...].reshape(rows, coherency.shape[3])
    product = jnp.dot(flat, swap[...], preferred_element_type=jnp.float32)
    turned[...] = product.astype(turned.dtype).reshape(turned.shape)


def swapped_pairs(coherency, interpret=False):
    rows, cols, channels, width = coherency.shape
    group = width // 8
    part = jnp.arange(width, dtype=jnp.int32)
    partner = part + jnp.where(part // group % 2 == 0, group, -group)
    swap = (part[:, None] == partner[None, :]).astype(coherency.dtype)
    block = pl.BlockSpec((SWAP_STEP, cols, channels, width), lambda s: (s, 0, 0, 0))
    return pl.pallas_call(
        swap_kernel,
        grid=(rows // SWAP_STEP,),
        in_specs=[block, pl.BlockSpec((width, width), lambda s: (0, 0))],
        out_specs=block,
        out_shape=jax.ShapeDtypeStruct(coherency.shape, coherency.dtype),
        compiler_params=pltpu.CompilerParams(dimension_semantics=("arbitrary",)),
        cost_estimate=pl.CostEstimate(
            flops=2 * width * coherency.size, bytes_accessed=4 * coherency.size, transcendentals=0
        ),
        interpret=interpret,
        name="swap",
    )(coherency, swap)


def gradients_kernel(
    gains,
    residual,
    coherency,
    turned,
    spread,
    sides,
    parts_even,
    parts_odd,
    sums_odd,
    col_parts,
    col_sums,
    weights_even,
    weights_odd,
    *,
    group,
):
    step = pl.program_id(0)
    per_step, col_count, channels, _ = coherency.shape
    row_count = residual.shape[0]
    lane = lax.broadcasted_iota(jnp.int32, (channels, LANES), 1)
    index = lane // group
    even = index % 2 == 0
    sign = jnp.where(even, -1.0, 1.0).astype(jnp.float32)

    def spread_out(row, weights):
        weights[...] = lax.dot_general(
            residual[row],
            spread[...],
            (((0,), (0,)), ((), ())),
            preferred_element_type=jnp.float32,
        )

    def prepare_row(row, parts):
        for b in (0, 1):
            own = gains[row, :, b * LANES : (b + 1) * LANES]
            for n in range(4):
                copies = replicas(own, group, index == n)
                parts[4 * b + n] = copies if n % 2 == 0 else sign * copies

    def finish_row(row, sums):
        for a in (0, 1):
            joined = None
            for n in range(4):
                own = sums[4 * a + n]
                part = summed_groups(own if n % 2 == 0 else sign * own, group)
                joined = part if n == 0 else jnp.where(index == n, part, joined)
            sides[row, :, a * LANES : (a + 1) * LANES] = joined

    @pl.when(step == 0)
    def _():
        col_sums[...] = jnp.zeros(col_sums.shape, col_sums.dtype)
        sums_odd[...] = jnp.zeros(sums_odd.shape, sums_odd.dtype)
        spread_out(0, weights_even)
        prepare_row(0, parts_even)

        def prepare_cols(block, carry):
            for j in range(BATCH):
                k = block * BATCH + j
                for b in (0, 1):
                    own = gains[row_count + k, :, b * LANES : (b + 1) * LANES]
                    col_parts[k, b] = own
                    col_parts[k, 2 + b] = sign * swapped(own, group, even)
            return carry

        lax.fori_loop(0, col_count // BATCH, prepare_cols, 0)

    def one_row(i, weights, parts):
        zero = jnp.zeros((channels, LANES), jnp.float32)
        sums = [zero] * 8
        for k in range(col_count):
            at = slice(k * channels, (k + 1) * channels)
            model = coherency[i, k].astype(jnp.float32)
            other = turned[i, k].astype(jnp.float32)
            m = [model[:, :LANES], model[:, LANES:]]
            sm = [other[:, :LANES], other[:, LANES:]]
            g = [weights[at, n * LANES : (n + 1) * LANES] for n in range(8)]
            for a in (0, 1):
                product = (
                    g[4 * a] * col_parts[k, 0]
                    + g[4 * a + 1] * col_parts[k, 2]
                    + g[4 * a + 2] * col_parts[k, 1]
                    + g[4 * a + 3] * col_parts[k, 3]
                )
                for c in (0, 1):
                    to = 4 * a + 2 * c
                    sums[to] = sums[to] + product * m[c]
                    sums[to + 1] = sums[to + 1] + product * sm[c]
            t = [
                parts[4 * b] * m[0]
                + parts[4 * b + 1] * sm[0]
                + parts[4 * b + 2] * m[1]
                + parts[4 * b + 3] * sm[1]
                for b in (0, 1)
            ]
            for a in (0, 1):
                col_sums[k, a] += g[2 * a] * t[0] + g[4 + 2 * a] * t[1]
                col_sums[k, 2 + a] += g[2 * a + 1] * t[0] + g[4 + 2 * a + 1] * t[1]
        return sums

    def two_rows(half, carry):
        i = 2 * half
        row = step * per_step + i
        following = jnp.minimum(row + 2, row_count - 1)
        finish_row(jnp.maximum(row - 1, 0), sums_odd)
        spread_out(row + 1, weights_odd)
        prepare_row(row + 1, parts_odd)
        finish_row(row, one_row(i, weights_even, parts_even))
        spread_out(following, weights_even)
        prepare_row(following, parts_even)
        sums = one_row(i + 1, weights_odd, parts_odd)
        for n in range(8):
            sums_odd[n] = sums[n]
        return carry

    lax.fori_loop(0, per_step // 2, two_rows, 0)

    @pl.when(step == pl.num_programs(0) - 1)
    def _():
        finish_row(row_count - 1, sums_odd)

        def finish_cols(block, carry):
            for j in range(BATCH):
                k = block * BATCH + j
                for a in (0, 1):
                    back = sign * swapped(col_sums[k, 2 + a], group, even)
                    to = slice(a * LANES, (a + 1) * LANES)
                    sides[row_count + k, :, to] = col_sums[k, a] - back
            return carry

        lax.fori_loop(0, col_count // BATCH, finish_cols, 0)


def block_gradients(coherency, turned, residual, gains, interpret=False):
    rows, cols, channels, width = coherency.shape
    lane = jnp.arange(8 * LANES, dtype=jnp.int32)
    spread = (lane[None, :8] == (lane[:, None] // LANES)).T.astype(jnp.bfloat16)
    block = pl.BlockSpec((PER_STEP, cols, channels, width), lambda s: (s, 0, 0, 0))
    whole = pl.BlockSpec((rows + cols, channels, width), lambda s: (0, 0, 0))
    return pl.pallas_call(
        functools.partial(gradients_kernel, group=width // 8),
        grid=(rows // PER_STEP,),
        in_specs=[
            whole,
            pl.BlockSpec((rows, 8, cols * channels), lambda s: (0, 0, 0)),
            block,
            block,
            pl.BlockSpec((8, 8 * LANES), lambda s: (0, 0)),
        ],
        out_specs=whole,
        out_shape=jax.ShapeDtypeStruct((rows + cols, channels, width), jnp.float32),
        scratch_shapes=[
            pltpu.VMEM((8, channels, LANES), jnp.float32),
            pltpu.VMEM((8, channels, LANES), jnp.float32),
            pltpu.VMEM((8, channels, LANES), jnp.float32),
            pltpu.VMEM((cols, 4, channels, LANES), jnp.float32),
            pltpu.VMEM((cols, 4, channels, LANES), jnp.float32),
            pltpu.VMEM((cols * channels, 8 * LANES), jnp.float32),
            pltpu.VMEM((cols * channels, 8 * LANES), jnp.float32),
        ],
        compiler_params=pltpu.CompilerParams(dimension_semantics=("arbitrary",)),
        interpret=interpret,
        name="gradients",
    )(gains, residual, coherency, turned, spread)


def weighted(cotangent, flags):
    rows, cols, channels = cotangent.shape[:3]
    kept = cotangent[:, :, :, 0, :] * flags.astype(cotangent.dtype)[:, :, :, None]
    return jnp.transpose(kept, (0, 3, 1, 2)).reshape(rows, 8, cols * channels)


def one_hot_product(table, values, dims):
    return lax.dot_general(
        table,
        values,
        (dims, ((), ())),
        precision=lax.Precision.HIGHEST,
        preferred_element_type=jnp.float32,
    )


def shards(gains, coherency, cotangent, flags, station_slot):
    stations = station_slot.shape[0]
    share, channels, width = gains.shape
    row_total = lax.axis_size("row")
    col_total = lax.axis_size("col")
    groups = row_total * col_total
    rows, cols = coherency.shape[:2]
    col_start = lax.axis_index("col") * cols

    by_channel = jnp.transpose(gains, (1, 0, 2))
    outward = jnp.broadcast_to(
        by_channel[:, None], (row_total, col_total, share, width)
    ).reshape(groups, share, width)
    channel_gains = exchanged(outward, ("row", "col"))
    models = coherency[:, :, :, 0, :]
    channel_gains, turned = lax.optimization_barrier((channel_gains, swapped_pairs(models)))
    channel_gains = channel_gains.reshape(stations, width)

    identity = jnp.arange(stations, dtype=jnp.int32)[None, :]
    table = (station_slot[:, None] == identity).astype(jnp.float32)
    slot_gains = one_hot_product(table, channel_gains, ((1,), (0,)))
    of_rows = slot_gains.reshape(row_total, rows, width)
    of_col = lax.dynamic_slice_in_dim(slot_gains, col_start, cols)
    of_cols = jnp.broadcast_to(of_col[None], (row_total, cols, width))
    needed = exchanged(jnp.concatenate([of_rows, of_cols], axis=1), "row")
    by_slot = jnp.transpose(needed, (1, 0, 2))

    sides = block_gradients(models, turned, weighted(cotangent, flags), by_slot)

    both = jnp.transpose(sides, (1, 0, 2))
    arrived = exchanged(both, "row")
    of_slots = arrived[:, :rows].reshape(stations, width)
    col_sum = jnp.sum(arrived[:, rows:], axis=0)
    mine = lax.dynamic_slice_in_dim(of_slots, col_start, cols)
    of_slots = lax.dynamic_update_slice_in_dim(of_slots, mine + col_sum, col_start, 0)
    of_stations = one_hot_product(table, of_slots, ((0,), (0,)))
    homeward = exchanged(of_stations.reshape(groups, share, width), ("row", "col"))
    total = jnp.sum(homeward.reshape(row_total, col_total, share, width), axis=1)
    return jnp.transpose(total, (1, 0, 2))


def solution(mesh):
    placed = (
        P(("row", "col"), None, None),
        P("row", "col", None, None, None),
        P("row", "col", None, None, None),
        P("row", "col", None),
        P(),
    )
    return jax.shard_map(
        shards, mesh=mesh, in_specs=placed, out_specs=P(("row", "col"), None, None), check_vma=False
    )
```

```python
import functools

import jax
import jax.numpy as jnp
from jax import lax
from jax.experimental import pallas as pl
from jax.experimental.pallas import tpu as pltpu
from jax.sharding import PartitionSpec as P

LANES = 128
PER_STEP = 8
SWAP_STEP = 16
BATCH = 8
VMEM_LIMIT = 24 * 1024 * 1024


def exchanged(x, axis):
    return lax.all_to_all(x, axis, split_axis=0, concat_axis=0, tiled=True)


def swapped(x, group, even):
    return jnp.where(even, pltpu.roll(x, LANES - group, 1), pltpu.roll(x, group, 1))


def summed_groups(x, group):
    half = x + pltpu.roll(x, 2 * group, 1)
    return half + pltpu.roll(half, group, 1)


def replicas(x, group, place):
    kept = jnp.where(place, x, 0.0)
    return summed_groups(kept, group)


def swap_kernel(coherency, swap, turned):
    rows = coherency.shape[0] * coherency.shape[1] * coherency.shape[2]
    flat = coherency[...].reshape(rows, coherency.shape[3])
    product = jnp.dot(flat, swap[...], preferred_element_type=jnp.float32)
    turned[...] = product.astype(turned.dtype).reshape(turned.shape)


def swapped_pairs(coherency, interpret=False):
    rows, cols, channels, width = coherency.shape
    group = width // 8
    part = jnp.arange(width, dtype=jnp.int32)
    partner = part + jnp.where(part // group % 2 == 0, group, -group)
    swap = (part[:, None] == partner[None, :]).astype(coherency.dtype)
    block = pl.BlockSpec((SWAP_STEP, cols, channels, width), lambda s: (s, 0, 0, 0))
    return pl.pallas_call(
        swap_kernel,
        grid=(rows // SWAP_STEP,),
        in_specs=[block, pl.BlockSpec((width, width), lambda s: (0, 0))],
        out_specs=block,
        out_shape=jax.ShapeDtypeStruct(coherency.shape, coherency.dtype),
        compiler_params=pltpu.CompilerParams(
            dimension_semantics=("arbitrary",), vmem_limit_bytes=VMEM_LIMIT
        ),
        cost_estimate=pl.CostEstimate(
            flops=2 * width * coherency.size, bytes_accessed=4 * coherency.size, transcendentals=0
        ),
        interpret=interpret,
        name="swap",
    )(coherency, swap)


def gradients_kernel(
    gains,
    residual,
    coherency,
    turned,
    spread,
    sides,
    parts_even,
    parts_odd,
    sums_odd,
    col_parts,
    col_sums,
    weights_even,
    weights_odd,
    *,
    group,
):
    step = pl.program_id(0)
    per_step, col_count, channels, _ = coherency.shape
    row_count = residual.shape[0]
    lane = lax.broadcasted_iota(jnp.int32, (channels, LANES), 1)
    index = lane // group
    even = index % 2 == 0
    sign = jnp.where(even, -1.0, 1.0).astype(jnp.float32)

    def spread_out(row, weights):
        weights[...] = lax.dot_general(
            residual[row],
            spread[...],
            (((0,), (0,)), ((), ())),
            preferred_element_type=jnp.float32,
        )

    def prepare_row(row, parts):
        for b in (0, 1):
            own = gains[row, :, b * LANES : (b + 1) * LANES]
            for n in range(4):
                copies = replicas(own, group, index == n)
                parts[4 * b + n] = copies if n % 2 == 0 else sign * copies

    def finish_row(row, sums):
        for a in (0, 1):
            joined = None
            for n in range(4):
                own = sums[4 * a + n]
                part = summed_groups(own if n % 2 == 0 else sign * own, group)
                joined = part if n == 0 else jnp.where(index == n, part, joined)
            sides[row, :, a * LANES : (a + 1) * LANES] = joined

    @pl.when(step == 0)
    def _():
        col_sums[...] = jnp.zeros(col_sums.shape, col_sums.dtype)
        sums_odd[...] = jnp.zeros(sums_odd.shape, sums_odd.dtype)
        spread_out(0, weights_even)
        prepare_row(0, parts_even)

        def prepare_cols(block, carry):
            for j in range(BATCH):
                k = block * BATCH + j
                for b in (0, 1):
                    own = gains[row_count + k, :, b * LANES : (b + 1) * LANES]
                    col_parts[k, b] = own
                    col_parts[k, 2 + b] = sign * swapped(own, group, even)
            return carry

        lax.fori_loop(0, col_count // BATCH, prepare_cols, 0)

    def one_row(i, weights, parts):
        zero = jnp.zeros((channels, LANES), jnp.float32)
        sums = [zero] * 8
        for k in range(col_count):
            at = slice(k * channels, (k + 1) * channels)
            model = coherency[i, k].astype(jnp.float32)
            other = turned[i, k].astype(jnp.float32)
            m = [model[:, :LANES], model[:, LANES:]]
            sm = [other[:, :LANES], other[:, LANES:]]
            g = [weights[at, n * LANES : (n + 1) * LANES] for n in range(8)]
            for a in (0, 1):
                product = (
                    g[4 * a] * col_parts[k, 0]
                    + g[4 * a + 1] * col_parts[k, 2]
                    + g[4 * a + 2] * col_parts[k, 1]
                    + g[4 * a + 3] * col_parts[k, 3]
                )
                for c in (0, 1):
                    to = 4 * a + 2 * c
                    sums[to] = sums[to] + product * m[c]
                    sums[to + 1] = sums[to + 1] + product * sm[c]
            t = [
                parts[4 * b] * m[0]
                + parts[4 * b + 1] * sm[0]
                + parts[4 * b + 2] * m[1]
                + parts[4 * b + 3] * sm[1]
                for b in (0, 1)
            ]
            for a in (0, 1):
                col_sums[k, a] += g[2 * a] * t[0] + g[4 + 2 * a] * t[1]
                col_sums[k, 2 + a] += g[2 * a + 1] * t[0] + g[4 + 2 * a + 1] * t[1]
        return sums

    def two_rows(half, carry):
        i = 2 * half
        row = step * per_step + i
        following = jnp.minimum(row + 2, row_count - 1)
        finish_row(jnp.maximum(row - 1, 0), sums_odd)
        spread_out(row + 1, weights_odd)
        prepare_row(row + 1, parts_odd)
        finish_row(row, one_row(i, weights_even, parts_even))
        spread_out(following, weights_even)
        prepare_row(following, parts_even)
        sums = one_row(i + 1, weights_odd, parts_odd)
        for n in range(8):
            sums_odd[n] = sums[n]
        return carry

    lax.fori_loop(0, per_step // 2, two_rows, 0)

    @pl.when(step == pl.num_programs(0) - 1)
    def _():
        finish_row(row_count - 1, sums_odd)

        def finish_cols(block, carry):
            for j in range(BATCH):
                k = block * BATCH + j
                for a in (0, 1):
                    back = sign * swapped(col_sums[k, 2 + a], group, even)
                    to = slice(a * LANES, (a + 1) * LANES)
                    sides[row_count + k, :, to] = col_sums[k, a] - back
            return carry

        lax.fori_loop(0, col_count // BATCH, finish_cols, 0)


def block_gradients(coherency, turned, residual, gains, interpret=False):
    rows, cols, channels, width = coherency.shape
    lane = jnp.arange(8 * LANES, dtype=jnp.int32)
    spread = (lane[None, :8] == (lane[:, None] // LANES)).T.astype(jnp.bfloat16)
    block = pl.BlockSpec((PER_STEP, cols, channels, width), lambda s: (s, 0, 0, 0))
    whole = pl.BlockSpec(memory_space=pltpu.VMEM)
    return pl.pallas_call(
        functools.partial(gradients_kernel, group=width // 8),
        grid=(rows // PER_STEP,),
        in_specs=[
            whole,
            whole,
            block,
            block,
            whole,
        ],
        out_specs=whole,
        out_shape=jax.ShapeDtypeStruct((rows + cols, channels, width), jnp.float32),
        scratch_shapes=[
            pltpu.VMEM((8, channels, LANES), jnp.float32),
            pltpu.VMEM((8, channels, LANES), jnp.float32),
            pltpu.VMEM((8, channels, LANES), jnp.float32),
            pltpu.VMEM((cols, 4, channels, LANES), jnp.float32),
            pltpu.VMEM((cols, 4, channels, LANES), jnp.float32),
            pltpu.VMEM((cols * channels, 8 * LANES), jnp.float32),
            pltpu.VMEM((cols * channels, 8 * LANES), jnp.float32),
        ],
        compiler_params=pltpu.CompilerParams(
            dimension_semantics=("arbitrary",), vmem_limit_bytes=VMEM_LIMIT
        ),
        interpret=interpret,
        name="gradients",
    )(gains, residual, coherency, turned, spread)


def weighted(cotangent, flags):
    rows, cols, channels = cotangent.shape[:3]
    kept = cotangent[:, :, :, 0, :] * flags.astype(cotangent.dtype)[:, :, :, None]
    return jnp.transpose(kept, (0, 3, 1, 2)).reshape(rows, 8, cols * channels)


def one_hot_product(table, values, dims):
    return lax.dot_general(
        table,
        values,
        (dims, ((), ())),
        precision=lax.Precision.HIGHEST,
        preferred_element_type=jnp.float32,
    )


def shards(gains, coherency, cotangent, flags, station_slot):
    stations = station_slot.shape[0]
    share, channels, width = gains.shape
    row_total = lax.axis_size("row")
    col_total = lax.axis_size("col")
    groups = row_total * col_total
    rows, cols = coherency.shape[:2]
    col_start = lax.axis_index("col") * cols

    by_channel = jnp.transpose(gains, (1, 0, 2))
    outward = jnp.broadcast_to(
        by_channel[:, None], (row_total, col_total, share, width)
    ).reshape(groups, share, width)
    channel_gains = exchanged(outward, ("row", "col"))
    models = coherency[:, :, :, 0, :]
    channel_gains, turned = lax.optimization_barrier((channel_gains, swapped_pairs(models)))
    channel_gains = channel_gains.reshape(stations, width)

    identity = jnp.arange(stations, dtype=jnp.int32)[None, :]
    table = (station_slot[:, None] == identity).astype(jnp.float32)
    slot_gains = one_hot_product(table, channel_gains, ((1,), (0,)))
    of_rows = slot_gains.reshape(row_total, rows, width)
    of_col = lax.dynamic_slice_in_dim(slot_gains, col_start, cols)
    of_cols = jnp.broadcast_to(of_col[None], (row_total, cols, width))
    needed = exchanged(jnp.concatenate([of_rows, of_cols], axis=1), "row")
    by_slot = jnp.transpose(needed, (1, 0, 2))

    sides = block_gradients(models, turned, weighted(cotangent, flags), by_slot)

    both = jnp.transpose(sides, (1, 0, 2))
    arrived = exchanged(both, "row")
    of_slots = arrived[:, :rows].reshape(stations, width)
    col_sum = jnp.sum(arrived[:, rows:], axis=0)
    mine = lax.dynamic_slice_in_dim(of_slots, col_start, cols)
    of_slots = lax.dynamic_update_slice_in_dim(of_slots, mine + col_sum, col_start, 0)
    of_stations = one_hot_product(table, of_slots, ((0,), (0,)))
    homeward = exchanged(of_stations.reshape(groups, share, width), ("row", "col"))
    total = jnp.sum(homeward.reshape(row_total, col_total, share, width), axis=1)
    return jnp.transpose(total, (1, 0, 2))


def solution(mesh):
    placed = (
        P(("row", "col"), None, None),
        P("row", "col", None, None, None),
        P("row", "col", None, None, None),
        P("row", "col", None),
        P(),
    )
    return jax.shard_map(
        shards, mesh=mesh, in_specs=placed, out_specs=P(("row", "col"), None, None), check_vma=False
    )
```

```python
import functools

import jax
import jax.numpy as jnp
from jax import lax
from jax.experimental import pallas as pl
from jax.experimental.pallas import tpu as pltpu
from jax.sharding import PartitionSpec as P

LANES = 128
PER_STEP = 4
SWAP_STEP = 16
BATCH = 8
VMEM_LIMIT = 48 * 1024 * 1024


def exchanged(x, axis):
    return lax.all_to_all(x, axis, split_axis=0, concat_axis=0, tiled=True)


def swapped(x, group, even):
    return jnp.where(even, pltpu.roll(x, LANES - group, 1), pltpu.roll(x, group, 1))


def summed_groups(x, group):
    half = x + pltpu.roll(x, 2 * group, 1)
    return half + pltpu.roll(half, group, 1)


def replicas(x, group, place):
    kept = jnp.where(place, x, 0.0)
    return summed_groups(kept, group)


def swap_kernel(coherency, swap, turned):
    rows = coherency.shape[0] * coherency.shape[1] * coherency.shape[2]
    flat = coherency[...].reshape(rows, coherency.shape[3])
    product = jnp.dot(flat, swap[...], preferred_element_type=jnp.float32)
    turned[...] = product.astype(turned.dtype).reshape(turned.shape)


def swapped_pairs(coherency, interpret=False):
    rows, cols, channels, width = coherency.shape
    group = width // 8
    part = jnp.arange(width, dtype=jnp.int32)
    partner = part + jnp.where(part // group % 2 == 0, group, -group)
    swap = (part[:, None] == partner[None, :]).astype(coherency.dtype)
    block = pl.BlockSpec((SWAP_STEP, cols, channels, width), lambda s: (s, 0, 0, 0))
    return pl.pallas_call(
        swap_kernel,
        grid=(rows // SWAP_STEP,),
        in_specs=[block, pl.BlockSpec((width, width), lambda s: (0, 0))],
        out_specs=block,
        out_shape=jax.ShapeDtypeStruct(coherency.shape, coherency.dtype),
        compiler_params=pltpu.CompilerParams(dimension_semantics=("arbitrary",)),
        cost_estimate=pl.CostEstimate(
            flops=2 * width * coherency.size, bytes_accessed=4 * coherency.size, transcendentals=0
        ),
        interpret=interpret,
        name="swap",
    )(coherency, swap)


def gradients_kernel(
    gains,
    residual,
    coherency,
    turned,
    spread,
    sides,
    parts_even,
    parts_odd,
    sums_odd,
    col_parts,
    col_sums,
    weights_even,
    weights_odd,
    model_slots,
    turned_slots,
    arrivals,
    *,
    group,
):
    row_count, col_count, channels, _ = coherency.shape
    steps = row_count // PER_STEP

    def fetches(step, slot):
        rows = pl.ds(step * PER_STEP, PER_STEP)
        return (
            pltpu.make_async_copy(coherency.at[rows], model_slots.at[slot], arrivals.at[0, slot]),
            pltpu.make_async_copy(turned.at[rows], turned_slots.at[slot], arrivals.at[1, slot]),
        )

    for ahead in (0, 1):
        for fetch in fetches(ahead, ahead):
            fetch.start()

    lane = lax.broadcasted_iota(jnp.int32, (channels, LANES), 1)
    index = lane // group
    even = index % 2 == 0
    sign = jnp.where(even, -1.0, 1.0).astype(jnp.float32)

    def spread_out(row, weights):
        weights[...] = lax.dot_general(
            residual[row],
            spread[...],
            (((0,), (0,)), ((), ())),
            preferred_element_type=jnp.float32,
        )

    def prepare_row(row, parts):
        for b in (0, 1):
            own = gains[row, :, b * LANES : (b + 1) * LANES]
            for n in range(4):
                copies = replicas(own, group, index == n)
                parts[4 * b + n] = copies if n % 2 == 0 else sign * copies

    def finish_row(row, sums):
        for a in (0, 1):
            joined = None
            for n in range(4):
                own = sums[4 * a + n]
                part = summed_groups(own if n % 2 == 0 else sign * own, group)
                joined = part if n == 0 else jnp.where(index == n, part, joined)
            sides[row, :, a * LANES : (a + 1) * LANES] = joined

    col_sums[...] = jnp.zeros(col_sums.shape, col_sums.dtype)
    sums_odd[...] = jnp.zeros(sums_odd.shape, sums_odd.dtype)
    spread_out(0, weights_even)
    prepare_row(0, parts_even)

    def prepare_cols(block, carry):
        for j in range(BATCH):
            k = block * BATCH + j
            for b in (0, 1):
                own = gains[row_count + k, :, b * LANES : (b + 1) * LANES]
                col_parts[k, b] = own
                col_parts[k, 2 + b] = sign * swapped(own, group, even)
        return carry

    lax.fori_loop(0, col_count // BATCH, prepare_cols, 0)

    def one_row(slot, i, weights, parts):
        zero = jnp.zeros((channels, LANES), jnp.float32)
        sums = [zero] * 8
        for k in range(col_count):
            at = slice(k * channels, (k + 1) * channels)
            model = model_slots[slot, i, k].astype(jnp.float32)
            other = turned_slots[slot, i, k].astype(jnp.float32)
            m = [model[:, :LANES], model[:, LANES:]]
            sm = [other[:, :LANES], other[:, LANES:]]
            g = [weights[at, n * LANES : (n + 1) * LANES] for n in range(8)]
            for a in (0, 1):
                product = (
                    g[4 * a] * col_parts[k, 0]
                    + g[4 * a + 1] * col_parts[k, 2]
                    + g[4 * a + 2] * col_parts[k, 1]
                    + g[4 * a + 3] * col_parts[k, 3]
                )
                for c in (0, 1):
                    to = 4 * a + 2 * c
                    sums[to] = sums[to] + product * m[c]
                    sums[to + 1] = sums[to + 1] + product * sm[c]
            t = [
                parts[4 * b] * m[0]
                + parts[4 * b + 1] * sm[0]
                + parts[4 * b + 2] * m[1]
                + parts[4 * b + 3] * sm[1]
                for b in (0, 1)
            ]
            for a in (0, 1):
                col_sums[k, a] += g[2 * a] * t[0] + g[4 + 2 * a] * t[1]
                col_sums[k, 2 + a] += g[2 * a + 1] * t[0] + g[4 + 2 * a + 1] * t[1]
        return sums

    def one_step(step, carry):
        slot = step % 2
        for fetch in fetches(step, slot):
            fetch.wait()

        def two_rows(half, inner):
            i = 2 * half
            row = step * PER_STEP + i
            following = jnp.minimum(row + 2, row_count - 1)
            finish_row(jnp.maximum(row - 1, 0), sums_odd)
            spread_out(row + 1, weights_odd)
            prepare_row(row + 1, parts_odd)
            finish_row(row, one_row(slot, i, weights_even, parts_even))
            spread_out(following, weights_even)
            prepare_row(following, parts_even)
            sums = one_row(slot, i + 1, weights_odd, parts_odd)
            for n in range(8):
                sums_odd[n] = sums[n]
            return inner

        lax.fori_loop(0, PER_STEP // 2, two_rows, 0)

        @pl.when(step + 2 < steps)
        def _():
            for fetch in fetches(step + 2, slot):
                fetch.start()

        return carry

    lax.fori_loop(0, steps, one_step, 0)
    finish_row(row_count - 1, sums_odd)

    def finish_cols(block, carry):
        for j in range(BATCH):
            k = block * BATCH + j
            for a in (0, 1):
                back = sign * swapped(col_sums[k, 2 + a], group, even)
                sides[row_count + k, :, a * LANES : (a + 1) * LANES] = col_sums[k, a] - back
        return carry

    lax.fori_loop(0, col_count // BATCH, finish_cols, 0)


def block_gradients(coherency, turned, residual, gains, interpret=False):
    rows, cols, channels, width = coherency.shape
    lane = jnp.arange(8 * LANES, dtype=jnp.int32)
    spread = (lane[None, :8] == (lane[:, None] // LANES)).T.astype(jnp.bfloat16)
    in_hbm = pl.BlockSpec(memory_space=pltpu.HBM)
    slots = pltpu.VMEM((2, PER_STEP, cols, channels, width), coherency.dtype)
    whole = pl.BlockSpec(memory_space=pltpu.VMEM)
    return pl.pallas_call(
        functools.partial(gradients_kernel, group=width // 8),
        in_specs=[
            whole,
            whole,
            in_hbm,
            in_hbm,
            whole,
        ],
        out_specs=whole,
        out_shape=jax.ShapeDtypeStruct((rows + cols, channels, width), jnp.float32),
        scratch_shapes=[
            pltpu.VMEM((8, channels, LANES), jnp.float32),
            pltpu.VMEM((8, channels, LANES), jnp.float32),
            pltpu.VMEM((8, channels, LANES), jnp.float32),
            pltpu.VMEM((cols, 4, channels, LANES), jnp.float32),
            pltpu.VMEM((cols, 4, channels, LANES), jnp.float32),
            pltpu.VMEM((cols * channels, 8 * LANES), jnp.float32),
            pltpu.VMEM((cols * channels, 8 * LANES), jnp.float32),
            slots,
            slots,
            pltpu.SemaphoreType.DMA((2, 2)),
        ],
        compiler_params=pltpu.CompilerParams(vmem_limit_bytes=VMEM_LIMIT),
        interpret=interpret,
        name="gradients",
    )(gains, residual, coherency, turned, spread)


def weighted(cotangent, flags):
    rows, cols, channels = cotangent.shape[:3]
    kept = cotangent[:, :, :, 0, :] * flags.astype(cotangent.dtype)[:, :, :, None]
    return jnp.transpose(kept, (0, 3, 1, 2)).reshape(rows, 8, cols * channels)


def one_hot_product(table, values, dims):
    return lax.dot_general(
        table,
        values,
        (dims, ((), ())),
        precision=lax.Precision.HIGHEST,
        preferred_element_type=jnp.float32,
    )


def shards(gains, coherency, cotangent, flags, station_slot):
    stations = station_slot.shape[0]
    share, channels, width = gains.shape
    row_total = lax.axis_size("row")
    col_total = lax.axis_size("col")
    groups = row_total * col_total
    rows, cols = coherency.shape[:2]
    col_start = lax.axis_index("col") * cols

    by_channel = jnp.transpose(gains, (1, 0, 2))
    outward = jnp.broadcast_to(
        by_channel[:, None], (row_total, col_total, share, width)
    ).reshape(groups, share, width)
    channel_gains = exchanged(outward, ("row", "col"))
    models = coherency[:, :, :, 0, :]
    channel_gains, turned = lax.optimization_barrier((channel_gains, swapped_pairs(models)))
    channel_gains = channel_gains.reshape(stations, width)

    identity = jnp.arange(stations, dtype=jnp.int32)[None, :]
    table = (station_slot[:, None] == identity).astype(jnp.float32)
    slot_gains = one_hot_product(table, channel_gains, ((1,), (0,)))
    of_rows = slot_gains.reshape(row_total, rows, width)
    of_col = lax.dynamic_slice_in_dim(slot_gains, col_start, cols)
    of_cols = jnp.broadcast_to(of_col[None], (row_total, cols, width))
    needed = exchanged(jnp.concatenate([of_rows, of_cols], axis=1), "row")
    by_slot = jnp.transpose(needed, (1, 0, 2))

    sides = block_gradients(models, turned, weighted(cotangent, flags), by_slot)

    both = jnp.transpose(sides, (1, 0, 2))
    arrived = exchanged(both, "row")
    of_slots = arrived[:, :rows].reshape(stations, width)
    col_sum = jnp.sum(arrived[:, rows:], axis=0)
    mine = lax.dynamic_slice_in_dim(of_slots, col_start, cols)
    of_slots = lax.dynamic_update_slice_in_dim(of_slots, mine + col_sum, col_start, 0)
    of_stations = one_hot_product(table, of_slots, ((0,), (0,)))
    homeward = exchanged(of_stations.reshape(groups, share, width), ("row", "col"))
    total = jnp.sum(homeward.reshape(row_total, col_total, share, width), axis=1)
    return jnp.transpose(total, (1, 0, 2))


def solution(mesh):
    placed = (
        P(("row", "col"), None, None),
        P("row", "col", None, None, None),
        P("row", "col", None, None, None),
        P("row", "col", None),
        P(),
    )
    return jax.shard_map(
        shards, mesh=mesh, in_specs=placed, out_specs=P(("row", "col"), None, None), check_vma=False
    )
```

```python
import functools

import jax
import jax.numpy as jnp
from jax import lax
from jax.experimental import pallas as pl
from jax.experimental.pallas import tpu as pltpu
from jax.sharding import PartitionSpec as P

LANES = 128
PER_STEP = 4
SWAP_STEP = 16
BATCH = 8
VMEM_LIMIT = 48 * 1024 * 1024


def exchanged(x, axis):
    return lax.all_to_all(x, axis, split_axis=0, concat_axis=0, tiled=True)


def swapped(x, group, even):
    return jnp.where(even, pltpu.roll(x, LANES - group, 1), pltpu.roll(x, group, 1))


def summed_groups(x, group):
    half = x + pltpu.roll(x, 2 * group, 1)
    return half + pltpu.roll(half, group, 1)


def replicas(x, group, place):
    kept = jnp.where(place, x, 0.0)
    return summed_groups(kept, group)


def swap_kernel(coherency, swap, turned):
    rows = coherency.shape[0] * coherency.shape[1] * coherency.shape[2]
    flat = coherency[...].reshape(rows, coherency.shape[3])
    product = jnp.dot(flat, swap[...], preferred_element_type=jnp.float32)
    turned[...] = product.astype(turned.dtype).reshape(turned.shape)


def swapped_pairs(coherency, interpret=False):
    rows, cols, channels, width = coherency.shape
    group = width // 8
    part = jnp.arange(width, dtype=jnp.int32)
    partner = part + jnp.where(part // group % 2 == 0, group, -group)
    swap = (part[:, None] == partner[None, :]).astype(coherency.dtype)
    block = pl.BlockSpec((SWAP_STEP, cols, channels, width), lambda s: (s, 0, 0, 0))
    return pl.pallas_call(
        swap_kernel,
        grid=(rows // SWAP_STEP,),
        in_specs=[block, pl.BlockSpec((width, width), lambda s: (0, 0))],
        out_specs=block,
        out_shape=jax.ShapeDtypeStruct(coherency.shape, coherency.dtype),
        compiler_params=pltpu.CompilerParams(dimension_semantics=("arbitrary",)),
        cost_estimate=pl.CostEstimate(
            flops=2 * width * coherency.size, bytes_accessed=4 * coherency.size, transcendentals=0
        ),
        interpret=interpret,
        name="swap",
    )(coherency, swap)


def gradients_kernel(
    gains,
    residual,
    coherency,
    turned,
    spread,
    sides,
    parts_even,
    parts_odd,
    sums_odd,
    col_parts,
    col_sums,
    weights_even,
    weights_odd,
    model_slots,
    turned_slots,
    arrivals,
    *,
    group,
):
    row_count, col_count, channels, _ = coherency.shape
    steps = row_count // PER_STEP

    def fetches(step, slot):
        rows = pl.ds(step * PER_STEP, PER_STEP)
        return (
            pltpu.make_async_copy(coherency.at[rows], model_slots.at[slot], arrivals.at[0, slot]),
            pltpu.make_async_copy(turned.at[rows], turned_slots.at[slot], arrivals.at[1, slot]),
        )

    for ahead in (0, 1):
        for fetch in fetches(ahead, ahead):
            fetch.start()

    lane = lax.broadcasted_iota(jnp.int32, (channels, LANES), 1)
    index = lane // group
    even = index % 2 == 0
    sign = jnp.where(even, -1.0, 1.0).astype(jnp.float32)

    def spread_out(row, weights):
        weights[...] = lax.dot_general(
            residual[row],
            spread[...],
            (((0,), (0,)), ((), ())),
            preferred_element_type=jnp.float32,
        )

    def prepare_row(row, parts):
        for b in (0, 1):
            own = gains[row, :, b * LANES : (b + 1) * LANES]
            for n in range(4):
                copies = replicas(own, group, index == n)
                parts[4 * b + n] = copies if n % 2 == 0 else sign * copies

    def finish_row(row, sums):
        for a in (0, 1):
            joined = None
            for n in range(4):
                own = sums[4 * a + n]
                part = summed_groups(own if n % 2 == 0 else sign * own, group)
                joined = part if n == 0 else jnp.where(index == n, part, joined)
            sides[row, :, a * LANES : (a + 1) * LANES] = joined

    col_sums[...] = jnp.zeros(col_sums.shape, col_sums.dtype)
    sums_odd[...] = jnp.zeros(sums_odd.shape, sums_odd.dtype)
    spread_out(0, weights_even)
    prepare_row(0, parts_even)

    def prepare_cols(block, carry):
        for j in range(BATCH):
            k = block * BATCH + j
            for b in (0, 1):
                own = gains[row_count + k, :, b * LANES : (b + 1) * LANES]
                col_parts[k, b] = own
                col_parts[k, 2 + b] = sign * swapped(own, group, even)
        return carry

    lax.fori_loop(0, col_count // BATCH, prepare_cols, 0)

    def one_row(slot, i, weights, parts):
        zero = jnp.zeros((channels, LANES), jnp.float32)
        sums = [zero] * 8
        for k in range(col_count):
            at = slice(k * channels, (k + 1) * channels)
            model = model_slots[slot, i, k].astype(jnp.float32)
            other = turned_slots[slot, i, k].astype(jnp.float32)
            m = [model[:, :LANES], model[:, LANES:]]
            sm = [other[:, :LANES], other[:, LANES:]]
            g = [weights[at, n * LANES : (n + 1) * LANES] for n in range(8)]
            for a in (0, 1):
                product = (
                    g[4 * a] * col_parts[k, 0]
                    + g[4 * a + 1] * col_parts[k, 2]
                    + g[4 * a + 2] * col_parts[k, 1]
                    + g[4 * a + 3] * col_parts[k, 3]
                )
                for c in (0, 1):
                    to = 4 * a + 2 * c
                    sums[to] = sums[to] + product * m[c]
                    sums[to + 1] = sums[to + 1] + product * sm[c]
            t = [
                parts[4 * b] * m[0]
                + parts[4 * b + 1] * sm[0]
                + parts[4 * b + 2] * m[1]
                + parts[4 * b + 3] * sm[1]
                for b in (0, 1)
            ]
            for a in (0, 1):
                col_sums[k, a] += g[2 * a] * t[0] + g[4 + 2 * a] * t[1]
                col_sums[k, 2 + a] += g[2 * a + 1] * t[0] + g[4 + 2 * a + 1] * t[1]
        return sums

    def one_step(step, carry):
        slot = step % 2
        for fetch in fetches(step, slot):
            fetch.wait()

        def two_rows(half, inner):
            i = 2 * half
            row = step * PER_STEP + i
            following = jnp.minimum(row + 2, row_count - 1)
            finish_row(jnp.maximum(row - 1, 0), sums_odd)
            spread_out(row + 1, weights_odd)
            prepare_row(row + 1, parts_odd)
            finish_row(row, one_row(slot, i, weights_even, parts_even))
            spread_out(following, weights_even)
            prepare_row(following, parts_even)
            sums = one_row(slot, i + 1, weights_odd, parts_odd)
            for n in range(8):
                sums_odd[n] = sums[n]
            return inner

        lax.fori_loop(0, PER_STEP // 2, two_rows, 0)

        @pl.when(step + 2 < steps)
        def _():
            for fetch in fetches(step + 2, slot):
                fetch.start()

        return carry

    lax.fori_loop(0, steps, one_step, 0)
    finish_row(row_count - 1, sums_odd)

    def finish_cols(block, carry):
        for j in range(BATCH):
            k = block * BATCH + j
            for a in (0, 1):
                back = sign * swapped(col_sums[k, 2 + a], group, even)
                sides[row_count + k, :, a * LANES : (a + 1) * LANES] = col_sums[k, a] - back
        return carry

    lax.fori_loop(0, col_count // BATCH, finish_cols, 0)


def block_gradients(coherency, turned, residual, gains, interpret=False):
    rows, cols, channels, width = coherency.shape
    lane = jnp.arange(8 * LANES, dtype=jnp.int32)
    spread = (lane[None, :8] == (lane[:, None] // LANES)).T.astype(jnp.bfloat16)
    in_hbm = pl.BlockSpec(memory_space=pltpu.HBM)
    slots = pltpu.VMEM((2, PER_STEP, cols, channels, width), coherency.dtype)
    whole = pl.BlockSpec(memory_space=pltpu.VMEM)
    return pl.pallas_call(
        functools.partial(gradients_kernel, group=width // 8),
        in_specs=[
            whole,
            whole,
            in_hbm,
            in_hbm,
            whole,
        ],
        out_specs=whole,
        out_shape=jax.ShapeDtypeStruct((rows + cols, channels, width), jnp.float32),
        scratch_shapes=[
            pltpu.VMEM((8, channels, LANES), jnp.float32),
            pltpu.VMEM((8, channels, LANES), jnp.float32),
            pltpu.VMEM((8, channels, LANES), jnp.float32),
            pltpu.VMEM((cols, 4, channels, LANES), jnp.float32),
            pltpu.VMEM((cols, 4, channels, LANES), jnp.float32),
            pltpu.VMEM((cols * channels, 8 * LANES), jnp.float32),
            pltpu.VMEM((cols * channels, 8 * LANES), jnp.float32),
            slots,
            slots,
            pltpu.SemaphoreType.DMA((2, 2)),
        ],
        compiler_params=pltpu.CompilerParams(
            vmem_limit_bytes=VMEM_LIMIT,
        ),
        interpret=interpret,
        name="gradients",
    )(gains, residual, coherency, turned, spread)


def weighted(cotangent, flags):
    rows, cols, channels = cotangent.shape[:3]
    kept = cotangent[:, :, :, 0, :] * flags.astype(cotangent.dtype)[:, :, :, None]
    return jnp.transpose(kept, (0, 3, 1, 2)).reshape(rows, 8, cols * channels)


def one_hot_product(table, values, dims):
    return lax.dot_general(
        table,
        values,
        (dims, ((), ())),
        precision=lax.Precision.HIGHEST,
        preferred_element_type=jnp.float32,
    )


def shards(gains, coherency, cotangent, flags, station_slot):
    stations = station_slot.shape[0]
    share, channels, width = gains.shape
    row_total = lax.axis_size("row")
    col_total = lax.axis_size("col")
    groups = row_total * col_total
    rows, cols = coherency.shape[:2]
    col_start = lax.axis_index("col") * cols

    by_channel = jnp.transpose(gains, (1, 0, 2))
    outward = jnp.broadcast_to(
        by_channel[:, None], (row_total, col_total, share, width)
    ).reshape(groups, share, width)
    channel_gains = exchanged(outward, ("row", "col"))
    models = coherency[:, :, :, 0, :]
    channel_gains, turned = lax.optimization_barrier((channel_gains, swapped_pairs(models)))
    channel_gains = channel_gains.reshape(stations, width)

    row_ids = station_slot.reshape(row_total, rows)
    col_ids = lax.dynamic_slice_in_dim(station_slot, col_start, cols)
    ids = jnp.concatenate(
        [row_ids, jnp.broadcast_to(col_ids[None], (row_total, cols))], axis=1
    ).reshape(-1)
    identity = jnp.arange(stations, dtype=jnp.int32)[None, :]
    outgoing = one_hot_product(
        (ids[:, None] == identity).astype(jnp.float32), channel_gains, ((1,), (0,))
    )
    needed = exchanged(outgoing.reshape(row_total, rows + cols, width), "row")
    by_slot = jnp.transpose(needed, (1, 0, 2))
    table = (station_slot[:, None] == identity).astype(jnp.float32)

    sides = block_gradients(models, turned, weighted(cotangent, flags), by_slot)

    both = jnp.transpose(sides, (1, 0, 2))
    arrived = exchanged(both, "row")
    of_slots = arrived[:, :rows].reshape(stations, width)
    col_sum = jnp.sum(arrived[:, rows:], axis=0)
    mine = lax.dynamic_slice_in_dim(of_slots, col_start, cols)
    of_slots = lax.dynamic_update_slice_in_dim(of_slots, mine + col_sum, col_start, 0)
    of_stations = one_hot_product(table, of_slots, ((0,), (0,)))
    homeward = exchanged(of_stations.reshape(groups, share, width), ("row", "col"))
    total = jnp.sum(homeward.reshape(row_total, col_total, share, width), axis=1)
    return jnp.transpose(total, (1, 0, 2))


def solution(mesh):
    placed = (
        P(("row", "col"), None, None),
        P("row", "col", None, None, None),
        P("row", "col", None, None, None),
        P("row", "col", None),
        P(),
    )
    return jax.shard_map(
        shards, mesh=mesh, in_specs=placed, out_specs=P(("row", "col"), None, None), check_vma=False
    )
```

```python
import functools

import jax
import jax.numpy as jnp
from jax import lax
from jax.experimental import pallas as pl
from jax.experimental.pallas import tpu as pltpu
from jax.sharding import PartitionSpec as P

LANES = 128
PER_STEP = 4
SWAP_STEP = 16
BATCH = 8
VMEM_LIMIT = 48 * 1024 * 1024


def exchanged(x, axis):
    return lax.all_to_all(x, axis, split_axis=0, concat_axis=0, tiled=True)


def swapped(x, group, even):
    return jnp.where(even, pltpu.roll(x, LANES - group, 1), pltpu.roll(x, group, 1))


def summed_groups(x, group):
    half = x + pltpu.roll(x, 2 * group, 1)
    return half + pltpu.roll(half, group, 1)


def replicas(x, group, place):
    kept = jnp.where(place, x, 0.0)
    return summed_groups(kept, group)


def swap_kernel(coherency, swap, turned):
    rows = coherency.shape[0] * coherency.shape[1] * coherency.shape[2]
    flat = coherency[...].reshape(rows, coherency.shape[3])
    product = jnp.dot(flat, swap[...], preferred_element_type=jnp.float32)
    turned[...] = product.astype(turned.dtype).reshape(turned.shape)


def swapped_pairs(coherency, interpret=False):
    rows, cols, channels, width = coherency.shape
    group = width // 8
    part = jnp.arange(width, dtype=jnp.int32)
    partner = part + jnp.where(part // group % 2 == 0, group, -group)
    swap = (part[:, None] == partner[None, :]).astype(coherency.dtype)
    block = pl.BlockSpec((SWAP_STEP, cols, channels, width), lambda s: (s, 0, 0, 0))
    return pl.pallas_call(
        swap_kernel,
        grid=(rows // SWAP_STEP,),
        in_specs=[block, pl.BlockSpec((width, width), lambda s: (0, 0))],
        out_specs=block,
        out_shape=jax.ShapeDtypeStruct(coherency.shape, coherency.dtype),
        compiler_params=pltpu.CompilerParams(dimension_semantics=("arbitrary",)),
        cost_estimate=pl.CostEstimate(
            flops=2 * width * coherency.size, bytes_accessed=4 * coherency.size, transcendentals=0
        ),
        interpret=interpret,
        name="swap",
    )(coherency, swap)


def gradients_kernel(
    gains,
    residual,
    coherency,
    turned,
    spread,
    sides,
    parts_even,
    parts_odd,
    sums_odd,
    col_parts,
    col_sums,
    weights_even,
    weights_odd,
    model_slots,
    turned_slots,
    arrivals,
    *,
    group,
):
    row_count, col_count, channels, _ = coherency.shape
    steps = row_count // PER_STEP

    def fetches(step, slot):
        rows = pl.ds(step * PER_STEP, PER_STEP)
        return (
            pltpu.make_async_copy(coherency.at[rows], model_slots.at[slot], arrivals.at[0, slot]),
            pltpu.make_async_copy(turned.at[rows], turned_slots.at[slot], arrivals.at[1, slot]),
        )

    for ahead in (0, 1):
        for fetch in fetches(ahead, ahead):
            fetch.start()

    lane = lax.broadcasted_iota(jnp.int32, (channels, LANES), 1)
    index = lane // group
    even = index % 2 == 0
    sign = jnp.where(even, -1.0, 1.0).astype(jnp.float32)

    slots = row_count + col_count

    def every_channel(slot, half):
        return pl.ds(half * slots + slot, channels, stride=2 * slots)

    def spread_out(row, weights):
        weights[...] = lax.dot_general(
            residual[row],
            spread[...],
            (((0,), (0,)), ((), ())),
            preferred_element_type=jnp.float32,
        )

    def prepare_row(row, parts):
        for b in (0, 1):
            own = gains[every_channel(row, b), :]
            for n in range(4):
                copies = replicas(own, group, index == n)
                parts[4 * b + n] = copies if n % 2 == 0 else sign * copies

    def finish_row(row, sums):
        for a in (0, 1):
            joined = None
            for n in range(4):
                own = sums[4 * a + n]
                part = summed_groups(own if n % 2 == 0 else sign * own, group)
                joined = part if n == 0 else jnp.where(index == n, part, joined)
            sides[every_channel(row, a), :] = joined

    col_sums[...] = jnp.zeros(col_sums.shape, col_sums.dtype)
    sums_odd[...] = jnp.zeros(sums_odd.shape, sums_odd.dtype)
    spread_out(0, weights_even)
    prepare_row(0, parts_even)

    def prepare_cols(block, carry):
        for j in range(BATCH):
            k = block * BATCH + j
            for b in (0, 1):
                own = gains[every_channel(row_count + k, b), :]
                col_parts[k, b] = own
                col_parts[k, 2 + b] = sign * swapped(own, group, even)
        return carry

    lax.fori_loop(0, col_count // BATCH, prepare_cols, 0)

    def one_row(slot, i, weights, parts):
        zero = jnp.zeros((channels, LANES), jnp.float32)
        sums = [zero] * 8
        for k in range(col_count):
            at = slice(k * channels, (k + 1) * channels)
            model = model_slots[slot, i, k].astype(jnp.float32)
            other = turned_slots[slot, i, k].astype(jnp.float32)
            m = [model[:, :LANES], model[:, LANES:]]
            sm = [other[:, :LANES], other[:, LANES:]]
            g = [weights[at, n * LANES : (n + 1) * LANES] for n in range(8)]
            for a in (0, 1):
                product = (
                    g[4 * a] * col_parts[k, 0]
                    + g[4 * a + 1] * col_parts[k, 2]
                    + g[4 * a + 2] * col_parts[k, 1]
                    + g[4 * a + 3] * col_parts[k, 3]
                )
                for c in (0, 1):
                    to = 4 * a + 2 * c
                    sums[to] = sums[to] + product * m[c]
                    sums[to + 1] = sums[to + 1] + product * sm[c]
            t = [
                parts[4 * b] * m[0]
                + parts[4 * b + 1] * sm[0]
                + parts[4 * b + 2] * m[1]
                + parts[4 * b + 3] * sm[1]
                for b in (0, 1)
            ]
            for a in (0, 1):
                col_sums[k, a] += g[2 * a] * t[0] + g[4 + 2 * a] * t[1]
                col_sums[k, 2 + a] += g[2 * a + 1] * t[0] + g[4 + 2 * a + 1] * t[1]
        return sums

    def one_step(step, carry):
        slot = step % 2
        for fetch in fetches(step, slot):
            fetch.wait()

        def two_rows(half, inner):
            i = 2 * half
            row = step * PER_STEP + i
            following = jnp.minimum(row + 2, row_count - 1)
            finish_row(jnp.maximum(row - 1, 0), sums_odd)
            spread_out(row + 1, weights_odd)
            prepare_row(row + 1, parts_odd)
            finish_row(row, one_row(slot, i, weights_even, parts_even))
            spread_out(following, weights_even)
            prepare_row(following, parts_even)
            sums = one_row(slot, i + 1, weights_odd, parts_odd)
            for n in range(8):
                sums_odd[n] = sums[n]
            return inner

        lax.fori_loop(0, PER_STEP // 2, two_rows, 0)

        @pl.when(step + 2 < steps)
        def _():
            for fetch in fetches(step + 2, slot):
                fetch.start()

        return carry

    lax.fori_loop(0, steps, one_step, 0)
    finish_row(row_count - 1, sums_odd)

    def finish_cols(block, carry):
        for j in range(BATCH):
            k = block * BATCH + j
            for a in (0, 1):
                back = sign * swapped(col_sums[k, 2 + a], group, even)
                sides[every_channel(row_count + k, a), :] = col_sums[k, a] - back
        return carry

    lax.fori_loop(0, col_count // BATCH, finish_cols, 0)


def block_gradients(coherency, turned, residual, gains, interpret=False):
    rows, cols, channels, width = coherency.shape
    lane = jnp.arange(8 * LANES, dtype=jnp.int32)
    spread = (lane[None, :8] == (lane[:, None] // LANES)).T.astype(jnp.bfloat16)
    in_hbm = pl.BlockSpec(memory_space=pltpu.HBM)
    slots = pltpu.VMEM((2, PER_STEP, cols, channels, width), coherency.dtype)
    whole = pl.BlockSpec(memory_space=pltpu.VMEM)
    return pl.pallas_call(
        functools.partial(gradients_kernel, group=width // 8),
        in_specs=[
            whole,
            whole,
            in_hbm,
            in_hbm,
            whole,
        ],
        out_specs=whole,
        out_shape=jax.ShapeDtypeStruct((channels * 2 * (rows + cols), LANES), jnp.float32),
        scratch_shapes=[
            pltpu.VMEM((8, channels, LANES), jnp.float32),
            pltpu.VMEM((8, channels, LANES), jnp.float32),
            pltpu.VMEM((8, channels, LANES), jnp.float32),
            pltpu.VMEM((cols, 4, channels, LANES), jnp.float32),
            pltpu.VMEM((cols, 4, channels, LANES), jnp.float32),
            pltpu.VMEM((cols * channels, 8 * LANES), jnp.float32),
            pltpu.VMEM((cols * channels, 8 * LANES), jnp.float32),
            slots,
            slots,
            pltpu.SemaphoreType.DMA((2, 2)),
        ],
        compiler_params=pltpu.CompilerParams(
            vmem_limit_bytes=VMEM_LIMIT,
        ),
        interpret=interpret,
        name="gradients",
    )(gains, residual, coherency, turned, spread)


def weighted(cotangent, flags):
    rows, cols, channels = cotangent.shape[:3]
    kept = cotangent[:, :, :, 0, :] * flags.astype(cotangent.dtype)[:, :, :, None]
    return jnp.transpose(kept, (0, 3, 1, 2)).reshape(rows, 8, cols * channels)


def exact_product(table, values):
    high = values.astype(jnp.bfloat16)
    rest = values - high.astype(jnp.float32)
    middle = rest.astype(jnp.bfloat16)
    low = (rest - middle.astype(jnp.float32)).astype(jnp.bfloat16)
    small = jnp.dot(table, low, preferred_element_type=jnp.float32)
    small += jnp.dot(table, middle, preferred_element_type=jnp.float32)
    return small + jnp.dot(table, high, preferred_element_type=jnp.float32)


def table_of(left, right):
    return jnp.where(left == right, 1.0, 0.0).astype(jnp.bfloat16)


def pack_kernel(identifiers, values, outgoing):
    row_total, _, slots, _ = outgoing.shape
    count, stations = identifiers.shape[0], values.shape[0]
    cols = count - stations
    rows = slots - cols
    station = lax.broadcasted_iota(jnp.int32, (count, stations), 1)
    ids = jnp.concatenate([identifiers[...]] * (stations // LANES), axis=1)
    chosen = exact_product(table_of(ids, station), values[...])
    for half in (0, 1):
        lanes = slice(half * LANES, (half + 1) * LANES)
        for r in range(row_total):
            outgoing[r, half, :rows] = chosen[r * rows : (r + 1) * rows, lanes]
            outgoing[r, half, rows:] = chosen[stations:, lanes]


def packed(identifiers, values, row_total, interpret=False):
    count, stations = identifiers.shape[0], values.shape[0]
    slots = stations // row_total + count - stations
    whole = pl.BlockSpec(memory_space=pltpu.VMEM)
    return pl.pallas_call(
        pack_kernel,
        in_specs=[whole, whole],
        out_specs=whole,
        out_shape=jax.ShapeDtypeStruct((row_total, 2, slots, LANES), jnp.float32),
        compiler_params=pltpu.CompilerParams(vmem_limit_bytes=VMEM_LIMIT),
        interpret=interpret,
        name="pack",
    )(identifiers, values)


def unpack_kernel(col_start, station_slot, arrived, sums, by_slot):
    row_total, _, slots, _ = arrived.shape
    stations = by_slot.shape[0]
    rows = stations // row_total
    cols = slots - rows
    mine = pl.ds(pl.multiple_of(col_start[0], cols), cols)
    for half in (0, 1):
        lanes = slice(half * LANES, (half + 1) * LANES)
        total = arrived[0, half, rows:]
        for r in range(row_total):
            by_slot[r * rows : (r + 1) * rows, lanes] = arrived[r, half, :rows]
            if r > 0:
                total = total + arrived[r, half, rows:]
        by_slot[mine, lanes] += total
    station = lax.broadcasted_iota(jnp.int32, (stations, stations), 0)
    sums[...] = exact_product(table_of(station_slot[...], station), by_slot[...])


def unpacked(col_start, station_slot, arrived, interpret=False):
    stations = station_slot.shape[1]
    whole = pl.BlockSpec(memory_space=pltpu.VMEM)
    return pl.pallas_call(
        unpack_kernel,
        in_specs=[pl.BlockSpec(memory_space=pltpu.SMEM), whole, whole],
        out_specs=whole,
        out_shape=jax.ShapeDtypeStruct((stations, 2 * LANES), jnp.float32),
        scratch_shapes=[pltpu.VMEM((stations, 2 * LANES), jnp.float32)],
        compiler_params=pltpu.CompilerParams(vmem_limit_bytes=VMEM_LIMIT),
        interpret=interpret,
        name="unpack",
    )(col_start, station_slot, arrived)


def shards(gains, coherency, cotangent, flags, station_slot):
    stations = station_slot.shape[0]
    share, channels, width = gains.shape
    row_total = lax.axis_size("row")
    col_total = lax.axis_size("col")
    groups = row_total * col_total
    rows, cols = coherency.shape[:2]
    col_start = lax.axis_index("col") * cols

    by_channel = jnp.transpose(gains, (1, 0, 2))
    outward = jnp.broadcast_to(
        by_channel[:, None], (row_total, col_total, share, width)
    ).reshape(groups, share, width)
    channel_gains = exchanged(outward, ("row", "col"))
    models = coherency[:, :, :, 0, :]
    col_ids = lax.dynamic_slice_in_dim(station_slot, col_start, cols)
    ids = jnp.concatenate([station_slot, col_ids])
    ids = jnp.broadcast_to(ids[:, None], (stations + cols, LANES))
    channel_gains, turned, ids = lax.optimization_barrier(
        (channel_gains, swapped_pairs(models), ids)
    )
    channel_gains = channel_gains.reshape(stations, width)

    outgoing = packed(ids, channel_gains, row_total)
    needed = exchanged(outgoing.reshape(row_total, -1, LANES), "row")

    sides = block_gradients(
        models, turned, weighted(cotangent, flags), needed.reshape(-1, LANES)
    )

    arrived = exchanged(sides.reshape(row_total, -1, LANES), "row")
    of_stations = unpacked(
        col_start.reshape(1),
        station_slot[None],
        arrived.reshape(row_total, 2, rows + cols, LANES),
    )
    homeward = exchanged(of_stations.reshape(groups, share, width), ("row", "col"))
    total = jnp.sum(homeward.reshape(row_total, col_total, share, width), axis=1)
    return jnp.transpose(total, (1, 0, 2))


def solution(mesh):
    placed = (
        P(("row", "col"), None, None),
        P("row", "col", None, None, None),
        P("row", "col", None, None, None),
        P("row", "col", None),
        P(),
    )
    return jax.shard_map(
        shards, mesh=mesh, in_specs=placed, out_specs=P(("row", "col"), None, None), check_vma=False
    )
```

```python
import functools

import jax
import jax.numpy as jnp
from jax import lax
from jax.experimental import pallas as pl
from jax.experimental.pallas import tpu as pltpu
from jax.sharding import PartitionSpec as P

LANES = 128
PER_STEP = 4
SWAP_STEP = 16
BATCH = 8
VMEM_LIMIT = 48 * 1024 * 1024


def exchanged(x, axis):
    return lax.all_to_all(x, axis, split_axis=0, concat_axis=0, tiled=True)


def swapped(x, group, even):
    return jnp.where(even, pltpu.roll(x, LANES - group, 1), pltpu.roll(x, group, 1))


def summed_groups(x, group):
    half = x + pltpu.roll(x, 2 * group, 1)
    return half + pltpu.roll(half, group, 1)


def replicas(x, group, place):
    kept = jnp.where(place, x, 0.0)
    return summed_groups(kept, group)


def swap_kernel(coherency, swap, turned):
    rows = coherency.shape[0] * coherency.shape[1] * coherency.shape[2]
    flat = coherency[...].reshape(rows, coherency.shape[3])
    product = jnp.dot(flat, swap[...], preferred_element_type=jnp.float32)
    turned[...] = product.astype(turned.dtype).reshape(turned.shape)


def swapped_pairs(coherency, interpret=False):
    rows, cols, channels, width = coherency.shape
    group = width // 8
    part = jnp.arange(width, dtype=jnp.int32)
    partner = part + jnp.where(part // group % 2 == 0, group, -group)
    swap = (part[:, None] == partner[None, :]).astype(coherency.dtype)
    block = pl.BlockSpec((SWAP_STEP, cols, channels, width), lambda s: (s, 0, 0, 0))
    return pl.pallas_call(
        swap_kernel,
        grid=(rows // SWAP_STEP,),
        in_specs=[block, pl.BlockSpec((width, width), lambda s: (0, 0))],
        out_specs=block,
        out_shape=jax.ShapeDtypeStruct(coherency.shape, coherency.dtype),
        compiler_params=pltpu.CompilerParams(dimension_semantics=("arbitrary",)),
        cost_estimate=pl.CostEstimate(
            flops=2 * width * coherency.size, bytes_accessed=4 * coherency.size, transcendentals=0
        ),
        interpret=interpret,
        name="swap",
    )(coherency, swap)


def gradients_kernel(
    half_index,
    kept,
    given,
    residual,
    coherency,
    turned,
    spread,
    own_sides,
    other_sides,
    parts_even,
    parts_odd,
    sums_odd,
    col_parts,
    col_sums,
    weights_even,
    weights_odd,
    model_slots,
    turned_slots,
    arrivals,
    *,
    group,
):
    row_count, col_count, channels, _ = coherency.shape
    half_count = row_count // 2
    steps = row_count // PER_STEP
    first_step = half_index[0] * (steps // 2)

    def fetches(step, slot):
        place = lax.rem(step + first_step, steps)
        rows = pl.ds(place * PER_STEP, PER_STEP)
        return (
            pltpu.make_async_copy(coherency.at[rows], model_slots.at[slot], arrivals.at[0, slot]),
            pltpu.make_async_copy(turned.at[rows], turned_slots.at[slot], arrivals.at[1, slot]),
        )

    for ahead in (0, 1):
        for fetch in fetches(ahead, ahead):
            fetch.start()

    lane = lax.broadcasted_iota(jnp.int32, (channels, LANES), 1)
    index = lane // group
    even = index % 2 == 0
    sign = jnp.where(even, -1.0, 1.0).astype(jnp.float32)

    slots = half_count + col_count

    def every_channel(slot, half):
        return pl.ds(half * slots + slot, channels, stride=2 * slots)

    def spread_out(row, weights):
        place = lax.rem(row + first_step * PER_STEP, row_count)
        weights[...] = lax.dot_general(
            residual[place],
            spread[...],
            (((0,), (0,)), ((), ())),
            preferred_element_type=jnp.float32,
        )

    def prepare_row(gains, row, parts):
        for b in (0, 1):
            own = gains[every_channel(row, b), :]
            for n in range(4):
                copies = replicas(own, group, index == n)
                parts[4 * b + n] = copies if n % 2 == 0 else sign * copies

    def finish_row(sides, row, sums):
        for a in (0, 1):
            joined = None
            for n in range(4):
                own = sums[4 * a + n]
                part = summed_groups(own if n % 2 == 0 else sign * own, group)
                joined = part if n == 0 else jnp.where(index == n, part, joined)
            sides[every_channel(row, a), :] = joined

    col_sums[...] = jnp.zeros(col_sums.shape, col_sums.dtype)
    sums_odd[...] = jnp.zeros(sums_odd.shape, sums_odd.dtype)
    spread_out(0, weights_even)
    prepare_row(kept, 0, parts_even)

    def prepare_cols(block, carry):
        for j in range(BATCH):
            k = block * BATCH + j
            for b in (0, 1):
                own = kept[every_channel(half_count + k, b), :]
                col_parts[k, b] = own
                col_parts[k, 2 + b] = sign * swapped(own, group, even)
        return carry

    lax.fori_loop(0, col_count // BATCH, prepare_cols, 0)

    def one_row(slot, i, weights, parts):
        zero = jnp.zeros((channels, LANES), jnp.float32)
        sums = [zero] * 8
        for k in range(col_count):
            at = slice(k * channels, (k + 1) * channels)
            model = model_slots[slot, i, k].astype(jnp.float32)
            other = turned_slots[slot, i, k].astype(jnp.float32)
            m = [model[:, :LANES], model[:, LANES:]]
            sm = [other[:, :LANES], other[:, LANES:]]
            g = [weights[at, n * LANES : (n + 1) * LANES] for n in range(8)]
            for a in (0, 1):
                product = (
                    g[4 * a] * col_parts[k, 0]
                    + g[4 * a + 1] * col_parts[k, 2]
                    + g[4 * a + 2] * col_parts[k, 1]
                    + g[4 * a + 3] * col_parts[k, 3]
                )
                for c in (0, 1):
                    to = 4 * a + 2 * c
                    sums[to] = sums[to] + product * m[c]
                    sums[to + 1] = sums[to + 1] + product * sm[c]
            t = [
                parts[4 * b] * m[0]
                + parts[4 * b + 1] * sm[0]
                + parts[4 * b + 2] * m[1]
                + parts[4 * b + 3] * sm[1]
                for b in (0, 1)
            ]
            for a in (0, 1):
                col_sums[k, a] += g[2 * a] * t[0] + g[4 + 2 * a] * t[1]
                col_sums[k, 2 + a] += g[2 * a + 1] * t[0] + g[4 + 2 * a + 1] * t[1]
        return sums

    def half_of_rows(gains, sides, start):
        def one_step(step, carry):
            slot = step % 2
            for fetch in fetches(step, slot):
                fetch.wait()

            def two_rows(half, inner):
                i = 2 * half
                row = step * PER_STEP + i
                at = row - start
                following = jnp.minimum(at + 2, half_count - 1)
                finish_row(sides, jnp.maximum(at - 1, 0), sums_odd)
                spread_out(row + 1, weights_odd)
                prepare_row(gains, at + 1, parts_odd)
                finish_row(sides, at, one_row(slot, i, weights_even, parts_even))
                spread_out(jnp.minimum(row + 2, row_count - 1), weights_even)
                prepare_row(gains, following, parts_even)
                sums = one_row(slot, i + 1, weights_odd, parts_odd)
                for n in range(8):
                    sums_odd[n] = sums[n]
                return inner

            lax.fori_loop(0, PER_STEP // 2, two_rows, 0)

            @pl.when(step + 2 < steps)
            def _():
                for fetch in fetches(step + 2, slot):
                    fetch.start()

            return carry

        first = start // PER_STEP
        lax.fori_loop(first, first + steps // 2, one_step, 0)
        finish_row(sides, half_count - 1, sums_odd)

    half_of_rows(kept, own_sides, 0)
    prepare_row(given, 0, parts_even)
    half_of_rows(given, other_sides, half_count)

    def finish_cols(block, carry):
        for j in range(BATCH):
            k = block * BATCH + j
            for a in (0, 1):
                back = sign * swapped(col_sums[k, 2 + a], group, even)
                own_sides[every_channel(half_count + k, a), :] = col_sums[k, a] - back
                other_sides[every_channel(half_count + k, a), :] = jnp.zeros_like(back)
        return carry

    lax.fori_loop(0, col_count // BATCH, finish_cols, 0)


def block_gradients(coherency, turned, residual, half_index, kept, given, interpret=False):
    rows, cols, channels, width = coherency.shape
    lane = jnp.arange(8 * LANES, dtype=jnp.int32)
    spread = (lane[None, :8] == (lane[:, None] // LANES)).T.astype(jnp.bfloat16)
    in_hbm = pl.BlockSpec(memory_space=pltpu.HBM)
    slots = pltpu.VMEM((2, PER_STEP, cols, channels, width), coherency.dtype)
    whole = pl.BlockSpec(memory_space=pltpu.VMEM)
    return pl.pallas_call(
        functools.partial(gradients_kernel, group=width // 8),
        in_specs=[
            pl.BlockSpec(memory_space=pltpu.SMEM),
            whole,
            whole,
            whole,
            in_hbm,
            in_hbm,
            whole,
        ],
        out_specs=[whole, whole],
        out_shape=[jax.ShapeDtypeStruct(kept.shape, jnp.float32)] * 2,
        scratch_shapes=[
            pltpu.VMEM((8, channels, LANES), jnp.float32),
            pltpu.VMEM((8, channels, LANES), jnp.float32),
            pltpu.VMEM((8, channels, LANES), jnp.float32),
            pltpu.VMEM((cols, 4, channels, LANES), jnp.float32),
            pltpu.VMEM((cols, 4, channels, LANES), jnp.float32),
            pltpu.VMEM((cols * channels, 8 * LANES), jnp.float32),
            pltpu.VMEM((cols * channels, 8 * LANES), jnp.float32),
            slots,
            slots,
            pltpu.SemaphoreType.DMA((2, 2)),
        ],
        compiler_params=pltpu.CompilerParams(
            vmem_limit_bytes=VMEM_LIMIT,
        ),
        interpret=interpret,
        name="gradients",
    )(half_index, kept, given, residual, coherency, turned, spread)


def weighted(cotangent, flags):
    rows, cols, channels = cotangent.shape[:3]
    kept = cotangent[:, :, :, 0, :] * flags.astype(cotangent.dtype)[:, :, :, None]
    return jnp.transpose(kept, (0, 3, 1, 2)).reshape(rows, 8, cols * channels)


def exact_product(table, values):
    high = values.astype(jnp.bfloat16)
    rest = values - high.astype(jnp.float32)
    middle = rest.astype(jnp.bfloat16)
    low = (rest - middle.astype(jnp.float32)).astype(jnp.bfloat16)
    small = jnp.dot(table, low, preferred_element_type=jnp.float32)
    small += jnp.dot(table, middle, preferred_element_type=jnp.float32)
    return small + jnp.dot(table, high, preferred_element_type=jnp.float32)


def table_of(left, right):
    return jnp.where(left == right, 1.0, 0.0).astype(jnp.bfloat16)


def pack_kernel(identifiers, values, outgoing):
    row_total, _, slots, _ = outgoing.shape
    count, stations = identifiers.shape[0], values.shape[0]
    rows = (count - slots) // (row_total - 1)
    cols = slots - rows
    station = lax.broadcasted_iota(jnp.int32, (count, stations), 1)
    ids = jnp.concatenate([identifiers[...]] * (stations // LANES), axis=1)
    chosen = exact_product(table_of(ids, station), values[...])
    for half in (0, 1):
        lanes = slice(half * LANES, (half + 1) * LANES)
        for r in range(row_total):
            outgoing[r, half, :rows] = chosen[r * rows : (r + 1) * rows, lanes]
            outgoing[r, half, rows:] = chosen[count - cols :, lanes]


def packed(identifiers, values, row_total, slots, interpret=False):
    whole = pl.BlockSpec(memory_space=pltpu.VMEM)
    return pl.pallas_call(
        pack_kernel,
        in_specs=[whole, whole],
        out_specs=whole,
        out_shape=jax.ShapeDtypeStruct((row_total, 2, slots, LANES), jnp.float32),
        compiler_params=pltpu.CompilerParams(vmem_limit_bytes=VMEM_LIMIT),
        interpret=interpret,
        name="pack",
    )(identifiers, values)


def unpack_kernel(starts, station_slot, arrived, sums, by_slot):
    row_total, _, slots, _ = arrived.shape
    stations = by_slot.shape[0]
    rows = stations // row_total // 2
    cols = slots - rows
    mine = pl.ds(pl.multiple_of(starts[0], cols), cols)
    by_slot[...] = jnp.zeros(by_slot.shape, by_slot.dtype)
    for half in (0, 1):
        lanes = slice(half * LANES, (half + 1) * LANES)
        total = arrived[0, half, rows:]
        for r in range(row_total):
            start = pl.multiple_of(2 * r * rows + starts[1] * rows, rows)
            by_slot[pl.ds(start, rows), lanes] = arrived[r, half, :rows]
            if r > 0:
                total = total + arrived[r, half, rows:]
        by_slot[mine, lanes] += total
    station = lax.broadcasted_iota(jnp.int32, (stations, stations), 0)
    sums[...] = exact_product(table_of(station_slot[...], station), by_slot[...])


def unpacked(starts, station_slot, arrived, interpret=False):
    stations = station_slot.shape[1]
    whole = pl.BlockSpec(memory_space=pltpu.VMEM)
    return pl.pallas_call(
        unpack_kernel,
        in_specs=[pl.BlockSpec(memory_space=pltpu.SMEM), whole, whole],
        out_specs=whole,
        out_shape=jax.ShapeDtypeStruct((stations, 2 * LANES), jnp.float32),
        scratch_shapes=[pltpu.VMEM((stations, 2 * LANES), jnp.float32)],
        compiler_params=pltpu.CompilerParams(vmem_limit_bytes=VMEM_LIMIT),
        interpret=interpret,
        name="unpack",
    )(starts, station_slot, arrived)


def shards(gains, coherency, cotangent, flags, station_slot):
    stations = station_slot.shape[0]
    share, channels, width = gains.shape
    row_total = lax.axis_size("row")
    col_total = lax.axis_size("col")
    groups = row_total * col_total
    rows, cols = coherency.shape[:2]
    col_start = lax.axis_index("col") * cols

    by_channel = jnp.transpose(gains, (1, 0, 2))
    outward = jnp.broadcast_to(
        by_channel[:, None], (row_total, col_total, share, width)
    ).reshape(groups, share, width)
    channel_gains = exchanged(outward, ("row", "col"))
    models = coherency[:, :, :, 0, :]
    half_index = lax.axis_index("col") % 2
    half = rows // 2
    row_ids = lax.dynamic_index_in_dim(
        station_slot.reshape(row_total, 2, half), half_index, 1, keepdims=False
    )
    col_ids = lax.dynamic_slice_in_dim(station_slot, col_start, cols)
    ids = jnp.concatenate([row_ids.reshape(-1), col_ids])
    ids = jnp.broadcast_to(ids[:, None], (ids.shape[0], LANES))
    channel_gains, turned, ids = lax.optimization_barrier(
        (channel_gains, swapped_pairs(models), ids)
    )
    channel_gains = channel_gains.reshape(stations, width)

    slots = half + cols
    pairs = [(i, i ^ 1) for i in range(col_total)]
    outgoing = packed(ids, channel_gains, row_total, slots)
    kept = exchanged(outgoing.reshape(row_total, -1, LANES), "row").reshape(-1, LANES)
    given = lax.ppermute(kept, "col", pairs)

    own, other = block_gradients(
        models, turned, weighted(cotangent, flags), half_index.reshape(1), kept, given
    )

    own = own + lax.ppermute(other, "col", pairs)
    arrived = exchanged(own.reshape(row_total, -1, LANES), "row")
    of_stations = unpacked(
        jnp.stack([col_start, half_index]),
        station_slot[None],
        arrived.reshape(row_total, 2, slots, LANES),
    )
    homeward = exchanged(of_stations.reshape(groups, share, width), ("row", "col"))
    total = jnp.sum(homeward.reshape(row_total, col_total, share, width), axis=1)
    return jnp.transpose(total, (1, 0, 2))


def solution(mesh):
    placed = (
        P(("row", "col"), None, None),
        P("row", "col", None, None, None),
        P("row", "col", None, None, None),
        P("row", "col", None),
        P(),
    )
    return jax.shard_map(
        shards, mesh=mesh, in_specs=placed, out_specs=P(("row", "col"), None, None), check_vma=False
    )
```

```python
import functools

import jax
import jax.numpy as jnp
from jax import lax
from jax.experimental import pallas as pl
from jax.experimental.pallas import tpu as pltpu
from jax.sharding import PartitionSpec as P

LANES = 128
PER_STEP = 4
SWAP_STEP = 16
BATCH = 8
VMEM_LIMIT = 48 * 1024 * 1024


def exchanged(x, axis):
    return lax.all_to_all(x, axis, split_axis=0, concat_axis=0, tiled=True)


def swapped(x, group, even):
    return jnp.where(even, pltpu.roll(x, LANES - group, 1), pltpu.roll(x, group, 1))


def summed_groups(x, group):
    half = x + pltpu.roll(x, 2 * group, 1)
    return half + pltpu.roll(half, group, 1)


def replicas(x, group, place):
    kept = jnp.where(place, x, 0.0)
    return summed_groups(kept, group)


def swap_kernel(coherency, swap, turned):
    rows = coherency.shape[0] * coherency.shape[1] * coherency.shape[2]
    flat = coherency[...].reshape(rows, coherency.shape[3])
    product = jnp.dot(flat, swap[...], preferred_element_type=jnp.float32)
    turned[...] = product.astype(turned.dtype).reshape(turned.shape)


def swapped_pairs(coherency, interpret=False):
    rows, cols, channels, width = coherency.shape
    group = width // 8
    part = jnp.arange(width, dtype=jnp.int32)
    partner = part + jnp.where(part // group % 2 == 0, group, -group)
    swap = (part[:, None] == partner[None, :]).astype(coherency.dtype)
    block = pl.BlockSpec((SWAP_STEP, cols, channels, width), lambda s: (s, 0, 0, 0))
    return pl.pallas_call(
        swap_kernel,
        grid=(rows // SWAP_STEP,),
        in_specs=[block, pl.BlockSpec((width, width), lambda s: (0, 0))],
        out_specs=block,
        out_shape=jax.ShapeDtypeStruct(coherency.shape, coherency.dtype),
        compiler_params=pltpu.CompilerParams(dimension_semantics=("arbitrary",)),
        cost_estimate=pl.CostEstimate(
            flops=2 * width * coherency.size, bytes_accessed=4 * coherency.size, transcendentals=0
        ),
        interpret=interpret,
        name="swap",
    )(coherency, swap)


def gradients_kernel(
    gains,
    residual,
    coherency,
    turned,
    spread,
    sides,
    parts_even,
    parts_odd,
    sums_odd,
    col_parts,
    col_sums,
    weights_even,
    weights_odd,
    model_slots,
    turned_slots,
    arrivals,
    *,
    group,
):
    row_count, col_count, channels, _ = coherency.shape
    steps = row_count // PER_STEP

    def fetches(step, slot):
        rows = pl.ds(step * PER_STEP, PER_STEP)
        return (
            pltpu.make_async_copy(coherency.at[rows], model_slots.at[slot], arrivals.at[0, slot]),
            pltpu.make_async_copy(turned.at[rows], turned_slots.at[slot], arrivals.at[1, slot]),
        )

    for ahead in (0, 1):
        for fetch in fetches(ahead, ahead):
            fetch.start()

    lane = lax.broadcasted_iota(jnp.int32, (channels, LANES), 1)
    index = lane // group
    even = index % 2 == 0
    sign = jnp.where(even, -1.0, 1.0).astype(jnp.float32)

    slots = row_count + col_count

    def every_channel(slot, half):
        return pl.ds(half * slots + slot, channels, stride=2 * slots)

    def spread_out(row, weights):
        weights[...] = lax.dot_general(
            residual[row],
            spread[...],
            (((0,), (0,)), ((), ())),
            preferred_element_type=jnp.float32,
        )

    def prepare_row(row, parts):
        for b in (0, 1):
            own = gains[every_channel(row, b), :]
            for n in range(4):
                copies = replicas(own, group, index == n)
                parts[4 * b + n] = copies if n % 2 == 0 else sign * copies

    def finish_row(row, sums):
        for a in (0, 1):
            joined = None
            for n in range(4):
                own = sums[4 * a + n]
                part = summed_groups(own if n % 2 == 0 else sign * own, group)
                joined = part if n == 0 else jnp.where(index == n, part, joined)
            sides[every_channel(row, a), :] = joined

    col_sums[...] = jnp.zeros(col_sums.shape, col_sums.dtype)
    sums_odd[...] = jnp.zeros(sums_odd.shape, sums_odd.dtype)
    spread_out(0, weights_even)
    prepare_row(0, parts_even)

    def prepare_cols(block, carry):
        for j in range(BATCH):
            k = block * BATCH + j
            for b in (0, 1):
                own = gains[every_channel(row_count + k, b), :]
                col_parts[k, b] = own
                col_parts[k, 2 + b] = sign * swapped(own, group, even)
        return carry

    lax.fori_loop(0, col_count // BATCH, prepare_cols, 0)

    def one_row(slot, i, weights, parts):
        zero = jnp.zeros((channels, LANES), jnp.float32)
        sums = [zero] * 8
        for k in range(col_count):
            at = slice(k * channels, (k + 1) * channels)
            model = model_slots[slot, i, k].astype(jnp.float32)
            other = turned_slots[slot, i, k].astype(jnp.float32)
            m = [model[:, :LANES], model[:, LANES:]]
            sm = [other[:, :LANES], other[:, LANES:]]
            g = [weights[at, n * LANES : (n + 1) * LANES] for n in range(8)]
            for a in (0, 1):
                product = (
                    g[4 * a] * col_parts[k, 0]
                    + g[4 * a + 1] * col_parts[k, 2]
                    + g[4 * a + 2] * col_parts[k, 1]
                    + g[4 * a + 3] * col_parts[k, 3]
                )
                for c in (0, 1):
                    to = 4 * a + 2 * c
                    sums[to] = sums[to] + product * m[c]
                    sums[to + 1] = sums[to + 1] + product * sm[c]
            t = [
                parts[4 * b] * m[0]
                + parts[4 * b + 1] * sm[0]
                + parts[4 * b + 2] * m[1]
                + parts[4 * b + 3] * sm[1]
                for b in (0, 1)
            ]
            for a in (0, 1):
                col_sums[k, a] += g[2 * a] * t[0] + g[4 + 2 * a] * t[1]
                col_sums[k, 2 + a] += g[2 * a + 1] * t[0] + g[4 + 2 * a + 1] * t[1]
        return sums

    def one_step(step, carry):
        slot = step % 2
        for fetch in fetches(step, slot):
            fetch.wait()

        def two_rows(half, inner):
            i = 2 * half
            row = step * PER_STEP + i
            following = jnp.minimum(row + 2, row_count - 1)
            finish_row(jnp.maximum(row - 1, 0), sums_odd)
            spread_out(row + 1, weights_odd)
            prepare_row(row + 1, parts_odd)
            finish_row(row, one_row(slot, i, weights_even, parts_even))
            spread_out(following, weights_even)
            prepare_row(following, parts_even)
            sums = one_row(slot, i + 1, weights_odd, parts_odd)
            for n in range(8):
                sums_odd[n] = sums[n]
            return inner

        lax.fori_loop(0, PER_STEP // 2, two_rows, 0)

        @pl.when(step + 2 < steps)
        def _():
            for fetch in fetches(step + 2, slot):
                fetch.start()

        return carry

    lax.fori_loop(0, steps, one_step, 0)
    finish_row(row_count - 1, sums_odd)

    def finish_cols(block, carry):
        for j in range(BATCH):
            k = block * BATCH + j
            for a in (0, 1):
                back = sign * swapped(col_sums[k, 2 + a], group, even)
                sides[every_channel(row_count + k, a), :] = col_sums[k, a] - back
        return carry

    lax.fori_loop(0, col_count // BATCH, finish_cols, 0)


def block_gradients(coherency, turned, residual, gains, interpret=False):
    rows, cols, channels, width = coherency.shape
    lane = jnp.arange(8 * LANES, dtype=jnp.int32)
    spread = (lane[None, :8] == (lane[:, None] // LANES)).T.astype(jnp.bfloat16)
    in_hbm = pl.BlockSpec(memory_space=pltpu.HBM)
    slots = pltpu.VMEM((2, PER_STEP, cols, channels, width), coherency.dtype)
    whole = pl.BlockSpec(memory_space=pltpu.VMEM)
    return pl.pallas_call(
        functools.partial(gradients_kernel, group=width // 8),
        in_specs=[
            whole,
            whole,
            in_hbm,
            in_hbm,
            whole,
        ],
        out_specs=whole,
        out_shape=jax.ShapeDtypeStruct((channels * 2 * (rows + cols), LANES), jnp.float32),
        scratch_shapes=[
            pltpu.VMEM((8, channels, LANES), jnp.float32),
            pltpu.VMEM((8, channels, LANES), jnp.float32),
            pltpu.VMEM((8, channels, LANES), jnp.float32),
            pltpu.VMEM((cols, 4, channels, LANES), jnp.float32),
            pltpu.VMEM((cols, 4, channels, LANES), jnp.float32),
            pltpu.VMEM((cols * channels, 8 * LANES), jnp.float32),
            pltpu.VMEM((cols * channels, 8 * LANES), jnp.float32),
            slots,
            slots,
            pltpu.SemaphoreType.DMA((2, 2)),
        ],
        compiler_params=pltpu.CompilerParams(
            vmem_limit_bytes=VMEM_LIMIT,
        ),
        interpret=interpret,
        name="gradients",
    )(gains, residual, coherency, turned, spread)


def weighted(cotangent, flags):
    rows, cols, channels = cotangent.shape[:3]
    kept = cotangent[:, :, :, 0, :] * flags.astype(cotangent.dtype)[:, :, :, None]
    return jnp.transpose(kept, (0, 3, 1, 2)).reshape(rows, 8, cols * channels)


def exact_product(table, values):
    high = values.astype(jnp.bfloat16)
    rest = values - high.astype(jnp.float32)
    middle = rest.astype(jnp.bfloat16)
    low = (rest - middle.astype(jnp.float32)).astype(jnp.bfloat16)
    small = jnp.dot(table, low, preferred_element_type=jnp.float32)
    small += jnp.dot(table, middle, preferred_element_type=jnp.float32)
    return small + jnp.dot(table, high, preferred_element_type=jnp.float32)


def table_of(left, right):
    return jnp.where(left == right, 1.0, 0.0).astype(jnp.bfloat16)


def pack_kernel(identifiers, values, outgoing):
    row_total, _, slots, _ = outgoing.shape
    count, stations = identifiers.shape[0], values.shape[0]
    cols = count - stations
    rows = slots - cols
    station = lax.broadcasted_iota(jnp.int32, (count, stations), 1)
    ids = jnp.concatenate([identifiers[...]] * (stations // LANES), axis=1)
    chosen = exact_product(table_of(ids, station), values[...])
    for half in (0, 1):
        lanes = slice(half * LANES, (half + 1) * LANES)
        for r in range(row_total):
            outgoing[r, half, :rows] = chosen[r * rows : (r + 1) * rows, lanes]
            outgoing[r, half, rows:] = chosen[stations:, lanes]


def packed(identifiers, values, row_total, interpret=False):
    count, stations = identifiers.shape[0], values.shape[0]
    slots = stations // row_total + count - stations
    whole = pl.BlockSpec(memory_space=pltpu.VMEM)
    return pl.pallas_call(
        pack_kernel,
        in_specs=[whole, whole],
        out_specs=whole,
        out_shape=jax.ShapeDtypeStruct((row_total, 2, slots, LANES), jnp.float32),
        compiler_params=pltpu.CompilerParams(vmem_limit_bytes=VMEM_LIMIT),
        interpret=interpret,
        name="pack",
    )(identifiers, values)


def outward_kernel(gains, outward):
    share, channels, _ = gains.shape
    copies = outward.shape[0] // channels
    for channel in range(channels):
        own = gains[:, channel, :]
        for copy in range(copies):
            outward[channel * copies + copy] = own


def outward_copies(gains, groups):
    share, _, width = gains.shape
    whole = pl.BlockSpec(memory_space=pltpu.VMEM)
    return pl.pallas_call(
        outward_kernel,
        in_specs=[whole],
        out_specs=whole,
        out_shape=jax.ShapeDtypeStruct((groups, share, width), jnp.float32),
        compiler_params=pltpu.CompilerParams(vmem_limit_bytes=VMEM_LIMIT),
        name="outward",
    )(gains)


def unpack_kernel(col_start, station_slot, arrived, sums, by_slot):
    row_total, _, slots, _ = arrived.shape
    stations = by_slot.shape[0]
    rows = stations // row_total
    cols = slots - rows
    mine = pl.ds(pl.multiple_of(col_start[0], cols), cols)
    for half in (0, 1):
        lanes = slice(half * LANES, (half + 1) * LANES)
        total = arrived[0, half, rows:]
        for r in range(row_total):
            by_slot[r * rows : (r + 1) * rows, lanes] = arrived[r, half, :rows]
            if r > 0:
                total = total + arrived[r, half, rows:]
        by_slot[mine, lanes] += total
    station = lax.broadcasted_iota(jnp.int32, (stations, stations), 0)
    sums[...] = exact_product(table_of(station_slot[...], station), by_slot[...])


def unpacked(col_start, station_slot, arrived, interpret=False):
    stations = station_slot.shape[1]
    whole = pl.BlockSpec(memory_space=pltpu.VMEM)
    return pl.pallas_call(
        unpack_kernel,
        in_specs=[pl.BlockSpec(memory_space=pltpu.SMEM), whole, whole],
        out_specs=whole,
        out_shape=jax.ShapeDtypeStruct((stations, 2 * LANES), jnp.float32),
        scratch_shapes=[pltpu.VMEM((stations, 2 * LANES), jnp.float32)],
        compiler_params=pltpu.CompilerParams(vmem_limit_bytes=VMEM_LIMIT),
        interpret=interpret,
        name="unpack",
    )(col_start, station_slot, arrived)


def shards(gains, coherency, cotangent, flags, station_slot):
    stations = station_slot.shape[0]
    share, channels, width = gains.shape
    row_total = lax.axis_size("row")
    col_total = lax.axis_size("col")
    groups = row_total * col_total
    rows, cols = coherency.shape[:2]
    col_start = lax.axis_index("col") * cols

    outward = outward_copies(gains, groups)
    channel_gains = exchanged(outward, ("row", "col"))
    models = coherency[:, :, :, 0, :]
    col_ids = lax.dynamic_slice_in_dim(station_slot, col_start, cols)
    ids = jnp.concatenate([station_slot, col_ids])
    ids = jnp.broadcast_to(ids[:, None], (stations + cols, LANES))
    channel_gains, turned, ids = lax.optimization_barrier(
        (channel_gains, swapped_pairs(models), ids)
    )
    channel_gains = channel_gains.reshape(stations, width)

    outgoing = packed(ids, channel_gains, row_total)
    needed = exchanged(outgoing.reshape(row_total, -1, LANES), "row")

    sides = block_gradients(
        models, turned, weighted(cotangent, flags), needed.reshape(-1, LANES)
    )

    arrived = exchanged(sides.reshape(row_total, -1, LANES), "row")
    of_stations = unpacked(
        col_start.reshape(1),
        station_slot[None],
        arrived.reshape(row_total, 2, rows + cols, LANES),
    )
    homeward = exchanged(of_stations.reshape(groups, share, width), ("row", "col"))
    total = jnp.sum(homeward.reshape(row_total, col_total, share, width), axis=1)
    return jnp.transpose(total, (1, 0, 2))


def solution(mesh):
    placed = (
        P(("row", "col"), None, None),
        P("row", "col", None, None, None),
        P("row", "col", None, None, None),
        P("row", "col", None),
        P(),
    )
    return jax.shard_map(
        shards, mesh=mesh, in_specs=placed, out_specs=P(("row", "col"), None, None), check_vma=False
    )
```

```python
import functools

import jax
import jax.numpy as jnp
from jax import lax
from jax.experimental import pallas as pl
from jax.experimental.pallas import tpu as pltpu
from jax.sharding import PartitionSpec as P

LANES = 128
PER_STEP = 4
SWAP_STEP = 16
BATCH = 8
VMEM_LIMIT = 48 * 1024 * 1024


def exchanged(x, axis):
    return lax.all_to_all(x, axis, split_axis=0, concat_axis=0, tiled=True)


def swapped(x, group, even):
    return jnp.where(even, pltpu.roll(x, LANES - group, 1), pltpu.roll(x, group, 1))


def summed_groups(x, group):
    half = x + pltpu.roll(x, 2 * group, 1)
    return half + pltpu.roll(half, group, 1)


def replicas(x, group, place):
    kept = jnp.where(place, x, 0.0)
    return summed_groups(kept, group)


def swap_kernel(coherency, swap, turned):
    rows = coherency.shape[0] * coherency.shape[1] * coherency.shape[2]
    flat = coherency[...].reshape(rows, coherency.shape[3])
    product = jnp.dot(flat, swap[...], preferred_element_type=jnp.float32)
    turned[...] = product.astype(turned.dtype).reshape(turned.shape)


def swapped_pairs(coherency, interpret=False):
    rows, cols, channels, width = coherency.shape
    group = width // 8
    part = jnp.arange(width, dtype=jnp.int32)
    partner = part + jnp.where(part // group % 2 == 0, group, -group)
    swap = (part[:, None] == partner[None, :]).astype(coherency.dtype)
    block = pl.BlockSpec((SWAP_STEP, cols, channels, width), lambda s: (s, 0, 0, 0))
    return pl.pallas_call(
        swap_kernel,
        grid=(rows // SWAP_STEP,),
        in_specs=[block, pl.BlockSpec((width, width), lambda s: (0, 0))],
        out_specs=block,
        out_shape=jax.ShapeDtypeStruct(coherency.shape, coherency.dtype),
        compiler_params=pltpu.CompilerParams(dimension_semantics=("arbitrary",)),
        cost_estimate=pl.CostEstimate(
            flops=2 * width * coherency.size, bytes_accessed=4 * coherency.size, transcendentals=0
        ),
        interpret=interpret,
        name="swap",
    )(coherency, swap)


def gradients_kernel(
    half_index,
    kept,
    given,
    residual,
    coherency,
    turned,
    spread,
    sides,
    parts_even,
    parts_odd,
    sums_odd,
    col_parts,
    col_sums,
    weights_even,
    weights_odd,
    model_slots,
    turned_slots,
    arrivals,
    *,
    group,
):
    row_count, col_count, channels, _ = coherency.shape
    steps = row_count // PER_STEP

    def fetches(step, slot):
        rows = pl.ds(step * PER_STEP, PER_STEP)
        return (
            pltpu.make_async_copy(coherency.at[rows], model_slots.at[slot], arrivals.at[0, slot]),
            pltpu.make_async_copy(turned.at[rows], turned_slots.at[slot], arrivals.at[1, slot]),
        )

    for ahead in (0, 1):
        for fetch in fetches(ahead, ahead):
            fetch.start()

    lane = lax.broadcasted_iota(jnp.int32, (channels, LANES), 1)
    index = lane // group
    even = index % 2 == 0
    sign = jnp.where(even, -1.0, 1.0).astype(jnp.float32)

    slots = row_count + col_count

    def every_channel(slot, half):
        return pl.ds(half * slots + slot, channels, stride=2 * slots)

    half_count = row_count // 2

    def gains_of(slot, half):
        reach = half_count + col_count
        return pl.ds(half * reach + slot, channels, stride=2 * reach)

    def spread_out(row, weights):
        weights[...] = lax.dot_general(
            residual[row],
            spread[...],
            (((0,), (0,)), ((), ())),
            preferred_element_type=jnp.float32,
        )

    def prepare_row(row, parts):
        for b in (0, 1):
            place = gains_of(lax.rem(row, half_count), b)
            own = jnp.where(row // half_count == half_index[0], kept[place, :], given[place, :])
            for n in range(4):
                copies = replicas(own, group, index == n)
                parts[4 * b + n] = copies if n % 2 == 0 else sign * copies

    def finish_row(row, sums):
        for a in (0, 1):
            joined = None
            for n in range(4):
                own = sums[4 * a + n]
                part = summed_groups(own if n % 2 == 0 else sign * own, group)
                joined = part if n == 0 else jnp.where(index == n, part, joined)
            sides[every_channel(row, a), :] = joined

    col_sums[...] = jnp.zeros(col_sums.shape, col_sums.dtype)
    sums_odd[...] = jnp.zeros(sums_odd.shape, sums_odd.dtype)
    spread_out(0, weights_even)
    prepare_row(0, parts_even)

    def prepare_cols(block, carry):
        for j in range(BATCH):
            k = block * BATCH + j
            for b in (0, 1):
                own = kept[gains_of(half_count + k, b), :]
                col_parts[k, b] = own
                col_parts[k, 2 + b] = sign * swapped(own, group, even)
        return carry

    lax.fori_loop(0, col_count // BATCH, prepare_cols, 0)

    def one_row(slot, i, weights, parts):
        zero = jnp.zeros((channels, LANES), jnp.float32)
        sums = [zero] * 8
        for k in range(col_count):
            at = slice(k * channels, (k + 1) * channels)
            model = model_slots[slot, i, k].astype(jnp.float32)
            other = turned_slots[slot, i, k].astype(jnp.float32)
            m = [model[:, :LANES], model[:, LANES:]]
            sm = [other[:, :LANES], other[:, LANES:]]
            g = [weights[at, n * LANES : (n + 1) * LANES] for n in range(8)]
            for a in (0, 1):
                product = (
                    g[4 * a] * col_parts[k, 0]
                    + g[4 * a + 1] * col_parts[k, 2]
                    + g[4 * a + 2] * col_parts[k, 1]
                    + g[4 * a + 3] * col_parts[k, 3]
                )
                for c in (0, 1):
                    to = 4 * a + 2 * c
                    sums[to] = sums[to] + product * m[c]
                    sums[to + 1] = sums[to + 1] + product * sm[c]
            t = [
                parts[4 * b] * m[0]
                + parts[4 * b + 1] * sm[0]
                + parts[4 * b + 2] * m[1]
                + parts[4 * b + 3] * sm[1]
                for b in (0, 1)
            ]
            for a in (0, 1):
                col_sums[k, a] += g[2 * a] * t[0] + g[4 + 2 * a] * t[1]
                col_sums[k, 2 + a] += g[2 * a + 1] * t[0] + g[4 + 2 * a + 1] * t[1]
        return sums

    def one_step(step, carry):
        slot = step % 2
        for fetch in fetches(step, slot):
            fetch.wait()

        def two_rows(half, inner):
            i = 2 * half
            row = step * PER_STEP + i
            following = jnp.minimum(row + 2, row_count - 1)
            finish_row(jnp.maximum(row - 1, 0), sums_odd)
            spread_out(row + 1, weights_odd)
            prepare_row(row + 1, parts_odd)
            finish_row(row, one_row(slot, i, weights_even, parts_even))
            spread_out(following, weights_even)
            prepare_row(following, parts_even)
            sums = one_row(slot, i + 1, weights_odd, parts_odd)
            for n in range(8):
                sums_odd[n] = sums[n]
            return inner

        lax.fori_loop(0, PER_STEP // 2, two_rows, 0)

        @pl.when(step + 2 < steps)
        def _():
            for fetch in fetches(step + 2, slot):
                fetch.start()

        return carry

    lax.fori_loop(0, steps, one_step, 0)
    finish_row(row_count - 1, sums_odd)

    def finish_cols(block, carry):
        for j in range(BATCH):
            k = block * BATCH + j
            for a in (0, 1):
                back = sign * swapped(col_sums[k, 2 + a], group, even)
                sides[every_channel(row_count + k, a), :] = col_sums[k, a] - back
        return carry

    lax.fori_loop(0, col_count // BATCH, finish_cols, 0)


def block_gradients(coherency, turned, residual, half_index, kept, given, interpret=False):
    rows, cols, channels, width = coherency.shape
    lane = jnp.arange(8 * LANES, dtype=jnp.int32)
    spread = (lane[None, :8] == (lane[:, None] // LANES)).T.astype(jnp.bfloat16)
    in_hbm = pl.BlockSpec(memory_space=pltpu.HBM)
    slots = pltpu.VMEM((2, PER_STEP, cols, channels, width), coherency.dtype)
    whole = pl.BlockSpec(memory_space=pltpu.VMEM)
    return pl.pallas_call(
        functools.partial(gradients_kernel, group=width // 8),
        in_specs=[
            pl.BlockSpec(memory_space=pltpu.SMEM),
            whole,
            whole,
            whole,
            in_hbm,
            in_hbm,
            whole,
        ],
        out_specs=whole,
        out_shape=jax.ShapeDtypeStruct((channels * 2 * (rows + cols), LANES), jnp.float32),
        scratch_shapes=[
            pltpu.VMEM((8, channels, LANES), jnp.float32),
            pltpu.VMEM((8, channels, LANES), jnp.float32),
            pltpu.VMEM((8, channels, LANES), jnp.float32),
            pltpu.VMEM((cols, 4, channels, LANES), jnp.float32),
            pltpu.VMEM((cols, 4, channels, LANES), jnp.float32),
            pltpu.VMEM((cols * channels, 8 * LANES), jnp.float32),
            pltpu.VMEM((cols * channels, 8 * LANES), jnp.float32),
            slots,
            slots,
            pltpu.SemaphoreType.DMA((2, 2)),
        ],
        compiler_params=pltpu.CompilerParams(
            vmem_limit_bytes=VMEM_LIMIT,
        ),
        interpret=interpret,
        name="gradients",
    )(half_index, kept, given, residual, coherency, turned, spread)


def weighted(cotangent, flags):
    rows, cols, channels = cotangent.shape[:3]
    kept = cotangent[:, :, :, 0, :] * flags.astype(cotangent.dtype)[:, :, :, None]
    return jnp.transpose(kept, (0, 3, 1, 2)).reshape(rows, 8, cols * channels)


def exact_product(table, values):
    high = values.astype(jnp.bfloat16)
    rest = values - high.astype(jnp.float32)
    middle = rest.astype(jnp.bfloat16)
    low = (rest - middle.astype(jnp.float32)).astype(jnp.bfloat16)
    small = jnp.dot(table, low, preferred_element_type=jnp.float32)
    small += jnp.dot(table, middle, preferred_element_type=jnp.float32)
    return small + jnp.dot(table, high, preferred_element_type=jnp.float32)


def table_of(left, right):
    return jnp.where(left == right, 1.0, 0.0).astype(jnp.bfloat16)


def pack_kernel(identifiers, values, outgoing):
    row_total, _, slots, _ = outgoing.shape
    count, stations = identifiers.shape[0], values.shape[0]
    rows = (count - slots) // (row_total - 1)
    cols = slots - rows
    station = lax.broadcasted_iota(jnp.int32, (count, stations), 1)
    ids = jnp.concatenate([identifiers[...]] * (stations // LANES), axis=1)
    chosen = exact_product(table_of(ids, station), values[...])
    for half in (0, 1):
        lanes = slice(half * LANES, (half + 1) * LANES)
        for r in range(row_total):
            outgoing[r, half, :rows] = chosen[r * rows : (r + 1) * rows, lanes]
            outgoing[r, half, rows:] = chosen[count - cols :, lanes]


def packed(identifiers, values, row_total, slots, interpret=False):
    whole = pl.BlockSpec(memory_space=pltpu.VMEM)
    return pl.pallas_call(
        pack_kernel,
        in_specs=[whole, whole],
        out_specs=whole,
        out_shape=jax.ShapeDtypeStruct((row_total, 2, slots, LANES), jnp.float32),
        compiler_params=pltpu.CompilerParams(vmem_limit_bytes=VMEM_LIMIT),
        interpret=interpret,
        name="pack",
    )(identifiers, values)


def unpack_kernel(col_start, station_slot, arrived, sums, by_slot):
    row_total, _, slots, _ = arrived.shape
    stations = by_slot.shape[0]
    rows = stations // row_total
    cols = slots - rows
    mine = pl.ds(pl.multiple_of(col_start[0], cols), cols)
    for half in (0, 1):
        lanes = slice(half * LANES, (half + 1) * LANES)
        total = arrived[0, half, rows:]
        for r in range(row_total):
            by_slot[r * rows : (r + 1) * rows, lanes] = arrived[r, half, :rows]
            if r > 0:
                total = total + arrived[r, half, rows:]
        by_slot[mine, lanes] += total
    station = lax.broadcasted_iota(jnp.int32, (stations, stations), 0)
    sums[...] = exact_product(table_of(station_slot[...], station), by_slot[...])


def unpacked(col_start, station_slot, arrived, interpret=False):
    stations = station_slot.shape[1]
    whole = pl.BlockSpec(memory_space=pltpu.VMEM)
    return pl.pallas_call(
        unpack_kernel,
        in_specs=[pl.BlockSpec(memory_space=pltpu.SMEM), whole, whole],
        out_specs=whole,
        out_shape=jax.ShapeDtypeStruct((stations, 2 * LANES), jnp.float32),
        scratch_shapes=[pltpu.VMEM((stations, 2 * LANES), jnp.float32)],
        compiler_params=pltpu.CompilerParams(vmem_limit_bytes=VMEM_LIMIT),
        interpret=interpret,
        name="unpack",
    )(col_start, station_slot, arrived)


def shards(gains, coherency, cotangent, flags, station_slot):
    stations = station_slot.shape[0]
    share, channels, width = gains.shape
    row_total = lax.axis_size("row")
    col_total = lax.axis_size("col")
    groups = row_total * col_total
    rows, cols = coherency.shape[:2]
    col_start = lax.axis_index("col") * cols

    by_channel = jnp.transpose(gains, (1, 0, 2))
    outward = jnp.broadcast_to(
        by_channel[:, None], (row_total, col_total, share, width)
    ).reshape(groups, share, width)
    channel_gains = exchanged(outward, ("row", "col"))
    models = coherency[:, :, :, 0, :]
    half_index = lax.axis_index("col") % 2
    half = rows // 2
    row_ids = lax.dynamic_index_in_dim(
        station_slot.reshape(row_total, 2, half), half_index, 1, keepdims=False
    )
    col_ids = lax.dynamic_slice_in_dim(station_slot, col_start, cols)
    ids = jnp.concatenate([row_ids.reshape(-1), col_ids])
    ids = jnp.broadcast_to(ids[:, None], (ids.shape[0], LANES))
    channel_gains, turned, ids = lax.optimization_barrier(
        (channel_gains, swapped_pairs(models), ids)
    )
    channel_gains = channel_gains.reshape(stations, width)

    outgoing = packed(ids, channel_gains, row_total, half + cols)
    kept = exchanged(outgoing.reshape(row_total, -1, LANES), "row").reshape(-1, LANES)
    given = lax.ppermute(kept, "col", [(i, i ^ 1) for i in range(col_total)])

    sides = block_gradients(
        models, turned, weighted(cotangent, flags), half_index.reshape(1), kept, given
    )

    arrived = exchanged(sides.reshape(row_total, -1, LANES), "row")
    of_stations = unpacked(
        col_start.reshape(1),
        station_slot[None],
        arrived.reshape(row_total, 2, rows + cols, LANES),
    )
    homeward = exchanged(of_stations.reshape(groups, share, width), ("row", "col"))
    total = jnp.sum(homeward.reshape(row_total, col_total, share, width), axis=1)
    return jnp.transpose(total, (1, 0, 2))


def solution(mesh):
    placed = (
        P(("row", "col"), None, None),
        P("row", "col", None, None, None),
        P("row", "col", None, None, None),
        P("row", "col", None),
        P(),
    )
    return jax.shard_map(
        shards, mesh=mesh, in_specs=placed, out_specs=P(("row", "col"), None, None), check_vma=False
    )
```

```python
import functools

import jax
import jax.numpy as jnp
from jax import lax
from jax.experimental import pallas as pl
from jax.experimental.pallas import tpu as pltpu
from jax.sharding import PartitionSpec as P

LANES = 128
PER_STEP = 4
SWAP_STEP = 16
BATCH = 8
VMEM_LIMIT = 48 * 1024 * 1024


def exchanged(x, axis):
    return lax.all_to_all(x, axis, split_axis=0, concat_axis=0, tiled=True)


def swapped(x, group, even):
    return jnp.where(even, pltpu.roll(x, LANES - group, 1), pltpu.roll(x, group, 1))


def summed_groups(x, group):
    half = x + pltpu.roll(x, 2 * group, 1)
    return half + pltpu.roll(half, group, 1)


def replicas(x, group, place):
    kept = jnp.where(place, x, 0.0)
    return summed_groups(kept, group)


def swap_kernel(coherency, swap, turned):
    rows = coherency.shape[0] * coherency.shape[1] * coherency.shape[2]
    flat = coherency[...].reshape(rows, coherency.shape[3])
    product = jnp.dot(flat, swap[...], preferred_element_type=jnp.float32)
    turned[...] = product.astype(turned.dtype).reshape(turned.shape)


def swapped_pairs(coherency, interpret=False):
    rows, cols, channels, width = coherency.shape
    group = width // 8
    part = jnp.arange(width, dtype=jnp.int32)
    partner = part + jnp.where(part // group % 2 == 0, group, -group)
    swap = (part[:, None] == partner[None, :]).astype(coherency.dtype)
    block = pl.BlockSpec((SWAP_STEP, cols, channels, width), lambda s: (s, 0, 0, 0))
    return pl.pallas_call(
        swap_kernel,
        grid=(rows // SWAP_STEP,),
        in_specs=[block, pl.BlockSpec((width, width), lambda s: (0, 0))],
        out_specs=block,
        out_shape=jax.ShapeDtypeStruct(coherency.shape, coherency.dtype),
        compiler_params=pltpu.CompilerParams(dimension_semantics=("arbitrary",)),
        cost_estimate=pl.CostEstimate(
            flops=2 * width * coherency.size, bytes_accessed=4 * coherency.size, transcendentals=0
        ),
        interpret=interpret,
        name="swap",
    )(coherency, swap)


def gradients_kernel(
    gains,
    residual,
    coherency,
    turned,
    spread,
    sides,
    parts_even,
    parts_odd,
    sums_odd,
    col_parts,
    col_sums,
    weights_even,
    weights_odd,
    model_slots,
    turned_slots,
    arrivals,
    *,
    group,
):
    row_count, col_count, channels, _ = coherency.shape
    steps = row_count // PER_STEP

    def fetches(step, slot):
        rows = pl.ds(step * PER_STEP, PER_STEP)
        return (
            pltpu.make_async_copy(coherency.at[rows], model_slots.at[slot], arrivals.at[0, slot]),
            pltpu.make_async_copy(turned.at[rows], turned_slots.at[slot], arrivals.at[1, slot]),
        )

    for ahead in (0, 1):
        for fetch in fetches(ahead, ahead):
            fetch.start()

    lane = lax.broadcasted_iota(jnp.int32, (channels, LANES), 1)
    index = lane // group
    even = index % 2 == 0
    sign = jnp.where(even, -1.0, 1.0).astype(jnp.float32)

    slots = row_count + col_count

    def every_channel(slot, half):
        return pl.ds(half * slots + slot, channels, stride=2 * slots)

    def spread_out(row, weights):
        weights[...] = lax.dot_general(
            residual[row],
            spread[...],
            (((0,), (0,)), ((), ())),
            preferred_element_type=jnp.float32,
        )

    def prepare_row(row, parts):
        for b in (0, 1):
            own = gains[every_channel(row, b), :]
            for n in range(4):
                copies = replicas(own, group, index == n)
                parts[4 * b + n] = copies if n % 2 == 0 else sign * copies

    def finish_row(row, sums):
        for a in (0, 1):
            joined = None
            for n in range(4):
                own = sums[4 * a + n]
                part = summed_groups(own if n % 2 == 0 else sign * own, group)
                joined = part if n == 0 else jnp.where(index == n, part, joined)
            sides[every_channel(row, a), :] = joined

    col_sums[...] = jnp.zeros(col_sums.shape, col_sums.dtype)
    sums_odd[...] = jnp.zeros(sums_odd.shape, sums_odd.dtype)
    spread_out(0, weights_even)
    prepare_row(0, parts_even)

    def prepare_cols(block, carry):
        for j in range(BATCH):
            k = block * BATCH + j
            for b in (0, 1):
                own = gains[every_channel(row_count + k, b), :]
                col_parts[k, b] = own
                col_parts[k, 2 + b] = sign * swapped(own, group, even)
        return carry

    lax.fori_loop(0, col_count // BATCH, prepare_cols, 0)

    def one_row(slot, i, weights, parts):
        zero = jnp.zeros((channels, LANES), jnp.float32)
        sums = [zero] * 8
        for k in range(col_count):
            at = slice(k * channels, (k + 1) * channels)
            model = model_slots[slot, i, k].astype(jnp.float32)
            other = turned_slots[slot, i, k].astype(jnp.float32)
            m = [model[:, :LANES], model[:, LANES:]]
            sm = [other[:, :LANES], other[:, LANES:]]
            g = [weights[at, n * LANES : (n + 1) * LANES] for n in range(8)]
            for a in (0, 1):
                product = (
                    g[4 * a] * col_parts[k, 0]
                    + g[4 * a + 1] * col_parts[k, 2]
                    + g[4 * a + 2] * col_parts[k, 1]
                    + g[4 * a + 3] * col_parts[k, 3]
                )
                for c in (0, 1):
                    to = 4 * a + 2 * c
                    sums[to] = sums[to] + product * m[c]
                    sums[to + 1] = sums[to + 1] + product * sm[c]
            t = [
                parts[4 * b] * m[0]
                + parts[4 * b + 1] * sm[0]
                + parts[4 * b + 2] * m[1]
                + parts[4 * b + 3] * sm[1]
                for b in (0, 1)
            ]
            for a in (0, 1):
                col_sums[k, a] += g[2 * a] * t[0] + g[4 + 2 * a] * t[1]
                col_sums[k, 2 + a] += g[2 * a + 1] * t[0] + g[4 + 2 * a + 1] * t[1]
        return sums

    def one_step(step, carry):
        slot = step % 2
        for fetch in fetches(step, slot):
            fetch.wait()

        def two_rows(half, inner):
            i = 2 * half
            row = step * PER_STEP + i
            following = jnp.minimum(row + 2, row_count - 1)
            finish_row(jnp.maximum(row - 1, 0), sums_odd)
            spread_out(row + 1, weights_odd)
            prepare_row(row + 1, parts_odd)
            finish_row(row, one_row(slot, i, weights_even, parts_even))
            spread_out(following, weights_even)
            prepare_row(following, parts_even)
            sums = one_row(slot, i + 1, weights_odd, parts_odd)
            for n in range(8):
                sums_odd[n] = sums[n]
            return inner

        lax.fori_loop(0, PER_STEP // 2, two_rows, 0)

        @pl.when(step + 2 < steps)
        def _():
            for fetch in fetches(step + 2, slot):
                fetch.start()

        return carry

    lax.fori_loop(0, steps, one_step, 0)
    finish_row(row_count - 1, sums_odd)

    def finish_cols(block, carry):
        for j in range(BATCH):
            k = block * BATCH + j
            for a in (0, 1):
                back = sign * swapped(col_sums[k, 2 + a], group, even)
                sides[every_channel(row_count + k, a), :] = col_sums[k, a] - back
        return carry

    lax.fori_loop(0, col_count // BATCH, finish_cols, 0)


def block_gradients(coherency, turned, residual, gains, interpret=False):
    rows, cols, channels, width = coherency.shape
    lane = jnp.arange(8 * LANES, dtype=jnp.int32)
    spread = (lane[None, :8] == (lane[:, None] // LANES)).T.astype(jnp.bfloat16)
    in_hbm = pl.BlockSpec(memory_space=pltpu.HBM)
    slots = pltpu.VMEM((2, PER_STEP, cols, channels, width), coherency.dtype)
    whole = pl.BlockSpec(memory_space=pltpu.VMEM)
    return pl.pallas_call(
        functools.partial(gradients_kernel, group=width // 8),
        in_specs=[
            whole,
            whole,
            in_hbm,
            in_hbm,
            whole,
        ],
        out_specs=whole,
        out_shape=jax.ShapeDtypeStruct((channels * 2 * (rows + cols), LANES), jnp.float32),
        scratch_shapes=[
            pltpu.VMEM((8, channels, LANES), jnp.float32),
            pltpu.VMEM((8, channels, LANES), jnp.float32),
            pltpu.VMEM((8, channels, LANES), jnp.float32),
            pltpu.VMEM((cols, 4, channels, LANES), jnp.float32),
            pltpu.VMEM((cols, 4, channels, LANES), jnp.float32),
            pltpu.VMEM((cols * channels, 8 * LANES), jnp.float32),
            pltpu.VMEM((cols * channels, 8 * LANES), jnp.float32),
            slots,
            slots,
            pltpu.SemaphoreType.DMA((2, 2)),
        ],
        compiler_params=pltpu.CompilerParams(
            vmem_limit_bytes=VMEM_LIMIT,
        ),
        interpret=interpret,
        name="gradients",
    )(gains, residual, coherency, turned, spread)


def weighted(cotangent, flags):
    rows, cols, channels = cotangent.shape[:3]
    kept = cotangent[:, :, :, 0, :] * flags.astype(cotangent.dtype)[:, :, :, None]
    return jnp.transpose(kept, (0, 3, 1, 2)).reshape(rows, 8, cols * channels)


def exact_product(table, values):
    high = values.astype(jnp.bfloat16)
    rest = values - high.astype(jnp.float32)
    middle = rest.astype(jnp.bfloat16)
    low = (rest - middle.astype(jnp.float32)).astype(jnp.bfloat16)
    small = jnp.dot(table, low, preferred_element_type=jnp.float32)
    small += jnp.dot(table, middle, preferred_element_type=jnp.float32)
    return small + jnp.dot(table, high, preferred_element_type=jnp.float32)


def table_of(left, right):
    return jnp.where(left == right, 1.0, 0.0).astype(jnp.bfloat16)


def pack_kernel(col_start, identifiers, values, outgoing, chosen):
    row_total, _, slots, _ = outgoing.shape
    stations = values.shape[0]
    rows = stations // row_total
    cols = slots - rows
    station = lax.broadcasted_iota(jnp.int32, (stations, stations), 1)
    ids = jnp.concatenate([identifiers[...]] * (stations // LANES), axis=1)
    chosen[...] = exact_product(table_of(ids, station), values[...])
    mine = pl.ds(pl.multiple_of(col_start[0], cols), cols)
    for half in (0, 1):
        lanes = slice(half * LANES, (half + 1) * LANES)
        for r in range(row_total):
            outgoing[r, half, :rows] = chosen[r * rows : (r + 1) * rows, lanes]
            outgoing[r, half, rows:] = chosen[mine, lanes]


def packed(col_start, identifiers, values, row_total, cols):
    stations, width = values.shape
    whole = pl.BlockSpec(memory_space=pltpu.VMEM)
    return pl.pallas_call(
        pack_kernel,
        in_specs=[pl.BlockSpec(memory_space=pltpu.SMEM), whole, whole],
        out_specs=whole,
        out_shape=jax.ShapeDtypeStruct(
            (row_total, 2, stations // row_total + cols, LANES), jnp.float32
        ),
        scratch_shapes=[pltpu.VMEM((stations, width), jnp.float32)],
        compiler_params=pltpu.CompilerParams(vmem_limit_bytes=VMEM_LIMIT),
        name="pack",
    )(col_start, identifiers, values)


def unpack_kernel(col_start, station_slot, arrived, sums, by_slot):
    row_total, _, slots, _ = arrived.shape
    stations = by_slot.shape[0]
    rows = stations // row_total
    cols = slots - rows
    mine = pl.ds(pl.multiple_of(col_start[0], cols), cols)
    for half in (0, 1):
        lanes = slice(half * LANES, (half + 1) * LANES)
        total = arrived[0, half, rows:]
        for r in range(row_total):
            by_slot[r * rows : (r + 1) * rows, lanes] = arrived[r, half, :rows]
            if r > 0:
                total = total + arrived[r, half, rows:]
        by_slot[mine, lanes] += total
    station = lax.broadcasted_iota(jnp.int32, (stations, stations), 0)
    sums[...] = exact_product(table_of(station_slot[...], station), by_slot[...])


def unpacked(col_start, station_slot, arrived, interpret=False):
    stations = station_slot.shape[1]
    whole = pl.BlockSpec(memory_space=pltpu.VMEM)
    return pl.pallas_call(
        unpack_kernel,
        in_specs=[pl.BlockSpec(memory_space=pltpu.SMEM), whole, whole],
        out_specs=whole,
        out_shape=jax.ShapeDtypeStruct((stations, 2 * LANES), jnp.float32),
        scratch_shapes=[pltpu.VMEM((stations, 2 * LANES), jnp.float32)],
        compiler_params=pltpu.CompilerParams(vmem_limit_bytes=VMEM_LIMIT),
        interpret=interpret,
        name="unpack",
    )(col_start, station_slot, arrived)


def shards(gains, coherency, cotangent, flags, station_slot):
    stations = station_slot.shape[0]
    share, channels, width = gains.shape
    row_total = lax.axis_size("row")
    col_total = lax.axis_size("col")
    groups = row_total * col_total
    rows, cols = coherency.shape[:2]
    col_start = lax.axis_index("col") * cols

    by_channel = jnp.transpose(gains, (1, 0, 2))
    outward = jnp.broadcast_to(
        by_channel[:, None], (row_total, col_total, share, width)
    ).reshape(groups, share, width)
    channel_gains = exchanged(outward, ("row", "col"))
    models = coherency[:, :, :, 0, :]
    ids = jnp.broadcast_to(station_slot[:, None], (stations, LANES))
    channel_gains, turned, ids = lax.optimization_barrier(
        (channel_gains, swapped_pairs(models), ids)
    )
    channel_gains = channel_gains.reshape(stations, width)

    outgoing = packed(col_start.reshape(1), ids, channel_gains, row_total, cols)
    needed = exchanged(outgoing.reshape(row_total, -1, LANES), "row")

    sides = block_gradients(
        models, turned, weighted(cotangent, flags), needed.reshape(-1, LANES)
    )

    arrived = exchanged(sides.reshape(row_total, -1, LANES), "row")
    of_stations = unpacked(
        col_start.reshape(1),
        station_slot[None],
        arrived.reshape(row_total, 2, rows + cols, LANES),
    )
    homeward = exchanged(of_stations.reshape(groups, share, width), ("row", "col"))
    total = jnp.sum(homeward.reshape(row_total, col_total, share, width), axis=1)
    return jnp.transpose(total, (1, 0, 2))


def solution(mesh):
    placed = (
        P(("row", "col"), None, None),
        P("row", "col", None, None, None),
        P("row", "col", None, None, None),
        P("row", "col", None),
        P(),
    )
    return jax.shard_map(
        shards, mesh=mesh, in_specs=placed, out_specs=P(("row", "col"), None, None), check_vma=False
    )
```

```python
import functools

import jax
import jax.numpy as jnp
from jax import lax
from jax.experimental import pallas as pl
from jax.experimental.pallas import tpu as pltpu
from jax.sharding import PartitionSpec as P

LANES = 128
PER_STEP = 4
SWAP_STEP = 16
BATCH = 8
VMEM_LIMIT = 48 * 1024 * 1024


def exchanged(x, axis):
    return lax.all_to_all(x, axis, split_axis=0, concat_axis=0, tiled=True)


def swapped(x, group, even):
    return jnp.where(even, pltpu.roll(x, LANES - group, 1), pltpu.roll(x, group, 1))


def summed_groups(x, group):
    half = x + pltpu.roll(x, 2 * group, 1)
    return half + pltpu.roll(half, group, 1)


def replicas(x, group, place):
    kept = jnp.where(place, x, 0.0)
    return summed_groups(kept, group)


def swap_kernel(coherency, turned):
    width = coherency.shape[3]
    group = width // 8
    part = lax.broadcasted_iota(jnp.int32, (width, width), 0)
    place = lax.broadcasted_iota(jnp.int32, (width, width), 1)
    partner = place + jnp.where(place // group % 2 == 0, group, -group)
    swap = jnp.where(part == partner, 1.0, 0.0).astype(coherency.dtype)
    rows = coherency.shape[0] * coherency.shape[1] * coherency.shape[2]
    flat = coherency[...].reshape(rows, coherency.shape[3])
    product = jnp.dot(flat, swap, preferred_element_type=jnp.float32)
    turned[...] = product.astype(turned.dtype).reshape(turned.shape)


def swapped_pairs(coherency, interpret=False):
    rows, cols, channels, width = coherency.shape
    block = pl.BlockSpec((SWAP_STEP, cols, channels, width), lambda s: (s, 0, 0, 0))
    return pl.pallas_call(
        swap_kernel,
        grid=(rows // SWAP_STEP,),
        in_specs=[block],
        out_specs=block,
        out_shape=jax.ShapeDtypeStruct(coherency.shape, coherency.dtype),
        compiler_params=pltpu.CompilerParams(dimension_semantics=("arbitrary",)),
        cost_estimate=pl.CostEstimate(
            flops=2 * width * coherency.size, bytes_accessed=4 * coherency.size, transcendentals=0
        ),
        interpret=interpret,
        name="swap",
    )(coherency)


def gradients_kernel(
    gains,
    residual,
    coherency,
    turned,
    spread,
    sides,
    parts_even,
    parts_odd,
    sums_odd,
    col_parts,
    col_sums,
    weights_even,
    weights_odd,
    model_slots,
    turned_slots,
    arrivals,
    *,
    group,
):
    row_count, col_count, channels, _ = coherency.shape
    steps = row_count // PER_STEP

    def fetches(step, slot):
        rows = pl.ds(step * PER_STEP, PER_STEP)
        return (
            pltpu.make_async_copy(coherency.at[rows], model_slots.at[slot], arrivals.at[0, slot]),
            pltpu.make_async_copy(turned.at[rows], turned_slots.at[slot], arrivals.at[1, slot]),
        )

    for ahead in (0, 1):
        for fetch in fetches(ahead, ahead):
            fetch.start()

    lane = lax.broadcasted_iota(jnp.int32, (channels, LANES), 1)
    index = lane // group
    even = index % 2 == 0
    sign = jnp.where(even, -1.0, 1.0).astype(jnp.float32)

    slots = row_count + col_count

    def every_channel(slot, half):
        return pl.ds(half * slots + slot, channels, stride=2 * slots)

    def spread_out(row, weights):
        weights[...] = lax.dot_general(
            residual[row],
            spread[...],
            (((0,), (0,)), ((), ())),
            preferred_element_type=jnp.float32,
        )

    def prepare_row(row, parts):
        for b in (0, 1):
            own = gains[every_channel(row, b), :]
            for n in range(4):
                copies = replicas(own, group, index == n)
                parts[4 * b + n] = copies if n % 2 == 0 else sign * copies

    def finish_row(row, sums):
        for a in (0, 1):
            joined = None
            for n in range(4):
                own = sums[4 * a + n]
                part = summed_groups(own if n % 2 == 0 else sign * own, group)
                joined = part if n == 0 else jnp.where(index == n, part, joined)
            sides[every_channel(row, a), :] = joined

    col_sums[...] = jnp.zeros(col_sums.shape, col_sums.dtype)
    sums_odd[...] = jnp.zeros(sums_odd.shape, sums_odd.dtype)
    spread_out(0, weights_even)
    prepare_row(0, parts_even)

    def prepare_cols(block, carry):
        for j in range(BATCH):
            k = block * BATCH + j
            for b in (0, 1):
                own = gains[every_channel(row_count + k, b), :]
                col_parts[k, b] = own
                col_parts[k, 2 + b] = sign * swapped(own, group, even)
        return carry

    lax.fori_loop(0, col_count // BATCH, prepare_cols, 0)

    def one_row(slot, i, weights, parts):
        zero = jnp.zeros((channels, LANES), jnp.float32)
        sums = [zero] * 8
        for k in range(col_count):
            at = slice(k * channels, (k + 1) * channels)
            model = model_slots[slot, i, k].astype(jnp.float32)
            other = turned_slots[slot, i, k].astype(jnp.float32)
            m = [model[:, :LANES], model[:, LANES:]]
            sm = [other[:, :LANES], other[:, LANES:]]
            g = [weights[at, n * LANES : (n + 1) * LANES] for n in range(8)]
            for a in (0, 1):
                product = (
                    g[4 * a] * col_parts[k, 0]
                    + g[4 * a + 1] * col_parts[k, 2]
                    + g[4 * a + 2] * col_parts[k, 1]
                    + g[4 * a + 3] * col_parts[k, 3]
                )
                for c in (0, 1):
                    to = 4 * a + 2 * c
                    sums[to] = sums[to] + product * m[c]
                    sums[to + 1] = sums[to + 1] + product * sm[c]
            t = [
                parts[4 * b] * m[0]
                + parts[4 * b + 1] * sm[0]
                + parts[4 * b + 2] * m[1]
                + parts[4 * b + 3] * sm[1]
                for b in (0, 1)
            ]
            for a in (0, 1):
                col_sums[k, a] += g[2 * a] * t[0] + g[4 + 2 * a] * t[1]
                col_sums[k, 2 + a] += g[2 * a + 1] * t[0] + g[4 + 2 * a + 1] * t[1]
        return sums

    def one_step(step, carry):
        slot = step % 2
        for fetch in fetches(step, slot):
            fetch.wait()

        def two_rows(half, inner):
            i = 2 * half
            row = step * PER_STEP + i
            following = jnp.minimum(row + 2, row_count - 1)
            finish_row(jnp.maximum(row - 1, 0), sums_odd)
            spread_out(row + 1, weights_odd)
            prepare_row(row + 1, parts_odd)
            finish_row(row, one_row(slot, i, weights_even, parts_even))
            spread_out(following, weights_even)
            prepare_row(following, parts_even)
            sums = one_row(slot, i + 1, weights_odd, parts_odd)
            for n in range(8):
                sums_odd[n] = sums[n]
            return inner

        lax.fori_loop(0, PER_STEP // 2, two_rows, 0)

        @pl.when(step + 2 < steps)
        def _():
            for fetch in fetches(step + 2, slot):
                fetch.start()

        return carry

    lax.fori_loop(0, steps, one_step, 0)
    finish_row(row_count - 1, sums_odd)

    def finish_cols(block, carry):
        for j in range(BATCH):
            k = block * BATCH + j
            for a in (0, 1):
                back = sign * swapped(col_sums[k, 2 + a], group, even)
                sides[every_channel(row_count + k, a), :] = col_sums[k, a] - back
        return carry

    lax.fori_loop(0, col_count // BATCH, finish_cols, 0)


def block_gradients(coherency, turned, residual, gains, interpret=False):
    rows, cols, channels, width = coherency.shape
    lane = jnp.arange(8 * LANES, dtype=jnp.int32)
    spread = (lane[None, :8] == (lane[:, None] // LANES)).T.astype(jnp.bfloat16)
    in_hbm = pl.BlockSpec(memory_space=pltpu.HBM)
    slots = pltpu.VMEM((2, PER_STEP, cols, channels, width), coherency.dtype)
    whole = pl.BlockSpec(memory_space=pltpu.VMEM)
    return pl.pallas_call(
        functools.partial(gradients_kernel, group=width // 8),
        in_specs=[
            whole,
            whole,
            in_hbm,
            in_hbm,
            whole,
        ],
        out_specs=whole,
        out_shape=jax.ShapeDtypeStruct((channels * 2 * (rows + cols), LANES), jnp.float32),
        scratch_shapes=[
            pltpu.VMEM((8, channels, LANES), jnp.float32),
            pltpu.VMEM((8, channels, LANES), jnp.float32),
            pltpu.VMEM((8, channels, LANES), jnp.float32),
            pltpu.VMEM((cols, 4, channels, LANES), jnp.float32),
            pltpu.VMEM((cols, 4, channels, LANES), jnp.float32),
            pltpu.VMEM((cols * channels, 8 * LANES), jnp.float32),
            pltpu.VMEM((cols * channels, 8 * LANES), jnp.float32),
            slots,
            slots,
            pltpu.SemaphoreType.DMA((2, 2)),
        ],
        compiler_params=pltpu.CompilerParams(
            vmem_limit_bytes=VMEM_LIMIT,
        ),
        interpret=interpret,
        name="gradients",
    )(gains, residual, coherency, turned, spread)


def weighted(cotangent, flags):
    rows, cols, channels = cotangent.shape[:3]
    kept = cotangent[:, :, :, 0, :] * flags.astype(cotangent.dtype)[:, :, :, None]
    return jnp.transpose(kept, (0, 3, 1, 2)).reshape(rows, 8, cols * channels)


def exact_product(table, values):
    high = values.astype(jnp.bfloat16)
    rest = values - high.astype(jnp.float32)
    middle = rest.astype(jnp.bfloat16)
    low = (rest - middle.astype(jnp.float32)).astype(jnp.bfloat16)
    small = jnp.dot(table, low, preferred_element_type=jnp.float32)
    small += jnp.dot(table, middle, preferred_element_type=jnp.float32)
    return small + jnp.dot(table, high, preferred_element_type=jnp.float32)


def table_of(left, right):
    return jnp.where(left == right, 1.0, 0.0).astype(jnp.bfloat16)


def pack_kernel(col_start, identifiers, values, outgoing, chosen):
    row_total, _, slots, _ = outgoing.shape
    stations = values.shape[0]
    rows = stations // row_total
    cols = slots - rows
    station = lax.broadcasted_iota(jnp.int32, (stations, stations), 1)
    ids = jnp.concatenate([identifiers[...]] * (stations // LANES), axis=1)
    chosen[...] = exact_product(table_of(ids, station), values[...])
    mine = pl.ds(pl.multiple_of(col_start[0], cols), cols)
    for half in (0, 1):
        lanes = slice(half * LANES, (half + 1) * LANES)
        for r in range(row_total):
            outgoing[r, half, :rows] = chosen[r * rows : (r + 1) * rows, lanes]
            outgoing[r, half, rows:] = chosen[mine, lanes]


def packed(col_start, identifiers, values, row_total, cols):
    stations, width = values.shape
    whole = pl.BlockSpec(memory_space=pltpu.VMEM)
    return pl.pallas_call(
        pack_kernel,
        in_specs=[pl.BlockSpec(memory_space=pltpu.SMEM), whole, whole],
        out_specs=whole,
        out_shape=jax.ShapeDtypeStruct(
            (row_total, 2, stations // row_total + cols, LANES), jnp.float32
        ),
        scratch_shapes=[pltpu.VMEM((stations, width), jnp.float32)],
        compiler_params=pltpu.CompilerParams(vmem_limit_bytes=VMEM_LIMIT),
        name="pack",
    )(col_start, identifiers, values)


def unpack_kernel(col_start, station_slot, arrived, sums, by_slot):
    row_total, _, slots, _ = arrived.shape
    stations = by_slot.shape[0]
    rows = stations // row_total
    cols = slots - rows
    mine = pl.ds(pl.multiple_of(col_start[0], cols), cols)
    for half in (0, 1):
        lanes = slice(half * LANES, (half + 1) * LANES)
        total = arrived[0, half, rows:]
        for r in range(row_total):
            by_slot[r * rows : (r + 1) * rows, lanes] = arrived[r, half, :rows]
            if r > 0:
                total = total + arrived[r, half, rows:]
        by_slot[mine, lanes] += total
    station = lax.broadcasted_iota(jnp.int32, (stations, stations), 0)
    sums[...] = exact_product(table_of(station_slot[...], station), by_slot[...])


def unpacked(col_start, station_slot, arrived, interpret=False):
    stations = station_slot.shape[1]
    whole = pl.BlockSpec(memory_space=pltpu.VMEM)
    return pl.pallas_call(
        unpack_kernel,
        in_specs=[pl.BlockSpec(memory_space=pltpu.SMEM), whole, whole],
        out_specs=whole,
        out_shape=jax.ShapeDtypeStruct((stations, 2 * LANES), jnp.float32),
        scratch_shapes=[pltpu.VMEM((stations, 2 * LANES), jnp.float32)],
        compiler_params=pltpu.CompilerParams(vmem_limit_bytes=VMEM_LIMIT),
        interpret=interpret,
        name="unpack",
    )(col_start, station_slot, arrived)


def shards(gains, coherency, cotangent, flags, station_slot):
    stations = station_slot.shape[0]
    share, channels, width = gains.shape
    row_total = lax.axis_size("row")
    col_total = lax.axis_size("col")
    groups = row_total * col_total
    rows, cols = coherency.shape[:2]
    col_start = lax.axis_index("col") * cols

    by_channel = jnp.transpose(gains, (1, 0, 2))
    outward = jnp.broadcast_to(
        by_channel[:, None], (row_total, col_total, share, width)
    ).reshape(groups, share, width)
    channel_gains = exchanged(outward, ("row", "col"))
    models = coherency[:, :, :, 0, :]
    ids = jnp.broadcast_to(station_slot[:, None], (stations, LANES))
    channel_gains, turned, ids = lax.optimization_barrier(
        (channel_gains, swapped_pairs(models), ids)
    )
    channel_gains = channel_gains.reshape(stations, width)

    outgoing = packed(col_start.reshape(1), ids, channel_gains, row_total, cols)
    needed = exchanged(outgoing.reshape(row_total, -1, LANES), "row")

    sides = block_gradients(
        models, turned, weighted(cotangent, flags), needed.reshape(-1, LANES)
    )

    arrived = exchanged(sides.reshape(row_total, -1, LANES), "row")
    of_stations = unpacked(
        col_start.reshape(1),
        station_slot[None],
        arrived.reshape(row_total, 2, rows + cols, LANES),
    )
    homeward = exchanged(of_stations.reshape(groups, share, width), ("row", "col"))
    total = jnp.sum(homeward.reshape(row_total, col_total, share, width), axis=1)
    return jnp.transpose(total, (1, 0, 2))


def solution(mesh):
    placed = (
        P(("row", "col"), None, None),
        P("row", "col", None, None, None),
        P("row", "col", None, None, None),
        P("row", "col", None),
        P(),
    )
    return jax.shard_map(
        shards, mesh=mesh, in_specs=placed, out_specs=P(("row", "col"), None, None), check_vma=False
    )
```
